16 devices in a mesh: dp: 4 (over y, z, core), sp: 4 (over x).
Axes of the slice: x: 4, y: 2, z: 1, core: 2. Of those that a mesh axis runs over, the one named last changes fastest.
The devices are a block of a 4x4x8 slice.
Arguments:
- x: bfloat16 [32768, 2048], P(('dp', 'sp')), parts along dimension 0
- gain: bfloat16 [2048], replicated
- wq: bfloat16 [2048, 2048], P('sp')
- wk: bfloat16 [2048, 2048], P('sp')
- wv: bfloat16 [2048, 2048], P('sp')
- wo: bfloat16 [2048, 2048], P('sp')
Outputs:
- output: bfloat16 [32768, 2048], P(('dp', 'sp')), parts along dimension 0
There are 4 independent parts. The reference program is written for one: setup_inputs(seed, part) draws one part's arguments, and reference() takes and returns one part's arrays. A program takes and returns all parts, laid end to end along the dimension named above; an argument that names none is the same for every part.
All inputs are finite; a program needn't handle non-finite values.
Results may differ from the reference program's by a relative error of at most 0.012.
Values are sent between devices in bfloat16 or wider.
A program may use at most 768 MiB of HBM per device.

```python
import jax
import jax.numpy as jnp
from jax import lax

ROWS = 8192
D = 2048
HEADS = 8
KV_HEADS = 8
HEAD = 256
THETA = 10000


def setup_inputs(seed: int = 0, part: int = 0) -> dict:
    kx, kn, kq, kk, kv, ko = jax.random.split(jax.random.key(seed), 6)

    def weights(key, rows, columns):
        return jax.random.normal(key, (rows, columns), jnp.float32) * rows**-0.5

    drawn = {
        "x": jax.random.normal(jax.random.fold_in(kx, part), (ROWS, D), jnp.float32),
        "gain": 1 + 0.1 * jax.random.normal(kn, (D,), jnp.float32),
        "wq": 2 * weights(kq, D, HEADS * HEAD),
        "wk": 2 * weights(kk, D, KV_HEADS * HEAD),
        "wv": 4 * weights(kv, D, KV_HEADS * HEAD),
        "wo": weights(ko, HEADS * HEAD, D),
    }
    return {k: v.astype(jnp.bfloat16) for k, v in drawn.items()}


def normed(x, gain):
    wide = x.astype(jnp.float32)
    scale = lax.rsqrt(jnp.mean(wide * wide, -1, keepdims=True) + 1e-6)
    return (wide * scale * gain.astype(jnp.float32)).astype(jnp.bfloat16)


def turned(t, place, theta):
    half = t.shape[-1] // 2
    angle = place.astype(jnp.float32)[:, None] * theta ** (-jnp.arange(half, dtype=jnp.float32) / half)
    cos, sin = jnp.cos(angle)[:, None], jnp.sin(angle)[:, None]
    a, b = t[..., :half].astype(jnp.float32), t[..., half:].astype(jnp.float32)
    return jnp.concatenate([a * cos - b * sin, b * cos + a * sin], -1).astype(jnp.bfloat16)


def matmul(a, w):
    return jnp.dot(a, w, preferred_element_type=jnp.float32).astype(jnp.bfloat16)


def einsum(form, a, b):
    return jnp.einsum(form, a.astype(jnp.float32), b.astype(jnp.float32))


def attention(q, k, v):
    scores = einsum("tgsd,ugd->gstu", q, k) * q.shape[-1] ** -0.5
    token = jnp.arange(q.shape[0])
    scores = jnp.where(token[:, None] >= token, scores, -jnp.inf)
    weights = jax.nn.softmax(scores, -1).astype(jnp.bfloat16)
    return einsum("gstu,ugd->tgsd", weights, v).astype(jnp.bfloat16)


def reference(x, gain, wq, wk, wv, wo):
    a, place = normed(x, gain), jnp.arange(ROWS)
    q = turned(matmul(a, wq).reshape(ROWS, HEADS, HEAD), place, THETA).reshape(ROWS, KV_HEADS, -1, HEAD)
    k = turned(matmul(a, wk).reshape(ROWS, KV_HEADS, HEAD), place, THETA)
    v = matmul(a, wv).reshape(ROWS, KV_HEADS, HEAD)
    seen = attention(q, k, v).reshape(ROWS, HEADS * HEAD)
    return (x.astype(jnp.float32) + jnp.dot(seen, wo, preferred_element_type=jnp.float32)).astype(jnp.bfloat16)
```

```python
import functools

import jax
import jax.numpy as jnp
from jax import lax
from jax.experimental import pallas as pl
from jax.experimental.pallas import tpu as pltpu
from jax.sharding import PartitionSpec as P

HEAD = 256
THETA = 10000
NEG = -1e30
HIDDEN = 2 * NEG
LOG2E = 1.4426950408889634
VMEM = 56 * 2**20
STRIP = 512
KEYS = 512
ROWS = 256


def _dot(a, b, ca, cb):
    return lax.dot_general(a, b, (((ca,), (cb,)), ((), ())), preferred_element_type=jnp.float32)


def _qkv_kernel(at_ref, x_ref, gain_ref, w_ref, cos_ref, sin_ref, *rest):
    q_ref, k_ref, vt_ref = rest[-3:]
    heads = q_ref.shape[0]
    half, width = HEAD // 2, heads * HEAD
    wide = x_ref[...].astype(jnp.float32)
    scale = lax.rsqrt(jnp.mean(wide * wide, -1, keepdims=True) + 1e-6)
    a = (wide * scale * gain_ref[...].astype(jnp.float32)).astype(jnp.bfloat16)
    cos, sin = cos_ref[...], sin_ref[...]
    for n, ref in enumerate((q_ref, k_ref)):
        t = _dot(a, w_ref[:, n * width : (n + 1) * width], 1, 0).astype(jnp.bfloat16).astype(jnp.float32)
        for h in range(heads):
            lo, hi = t[:, h * HEAD : h * HEAD + half], t[:, h * HEAD + half : (h + 1) * HEAD]
            ref[h, :, :half] = (lo * cos - hi * sin).astype(jnp.bfloat16)
            ref[h, :, half:] = (hi * cos + lo * sin).astype(jnp.bfloat16)
    v = _dot(a, w_ref[:, 2 * width :], 1, 0).astype(jnp.bfloat16)
    for h in range(heads):
        vt_ref[h] = v[:, h * HEAD : (h + 1) * HEAD].T


def qkv(first, x, gain, w, cos, sin, bufs):
    rows, depth = x.shape
    heads = w.shape[1] // (3 * HEAD)
    shapes = [(heads, len(cos), HEAD), (heads, len(cos), HEAD), (heads, HEAD, len(cos))]
    at = (first // ROWS).astype(jnp.int32).reshape(1)
    table = pl.BlockSpec((ROWS, HEAD // 2), lambda r, at: (at[0] + r, 0))
    anywhere = pl.BlockSpec(memory_space=pl.ANY)
    tokens = pl.BlockSpec((heads, ROWS, HEAD), lambda r, at: (0, at[0] + r, 0))
    return pl.pallas_call(
        _qkv_kernel,
        grid_spec=pltpu.PrefetchScalarGridSpec(
            num_scalar_prefetch=1,
            grid=(rows // ROWS,),
            in_specs=[
                pl.BlockSpec((ROWS, depth), lambda r, at: (r, 0)),
                pl.BlockSpec((1, depth), lambda r, at: (0, 0)),
                pl.BlockSpec(w.shape, lambda r, at: (0, 0), pipeline_mode=pl.Buffered(1)),
                table,
                table,
                *[anywhere] * len(bufs),
            ],
            out_specs=[tokens, tokens, pl.BlockSpec((heads, HEAD, ROWS), lambda r, at: (0, 0, at[0] + r))],
        ),
        out_shape=[jax.ShapeDtypeStruct(s, x.dtype) for s in shapes],
        input_output_aliases={6 + i: i for i in range(len(bufs))},
        compiler_params=pltpu.CompilerParams(dimension_semantics=("arbitrary",), vmem_limit_bytes=VMEM),
        cost_estimate=pl.CostEstimate(
            flops=2 * rows * depth * w.shape[1], transcendentals=0, bytes_accessed=2 * (rows * depth + w.size + rows * w.shape[1])
        ),
        name="qkv",
    )(at, x, gain, w, cos, sin, *bufs)


def _attend_kernel(tab_ref, q_ref, k_ref, vt_ref, *rest, scale, steps, carried, kept):
    st_in = rest[0] if carried else None
    o_ref = rest[carried]
    st_out = rest[carried + 1] if kept else None
    top_s, mix_s = rest[-2:]
    heads, cols = q_ref.shape[0], q_ref.shape[1]
    r, c = pl.program_id(0), pl.program_id(1)
    mode = tab_ref[pl.num_programs(0) * (1 + steps) + r * steps + c]
    e = scale * LOG2E
    low = jnp.bfloat16
    strips = cols // STRIP
    ones = jnp.ones((8, KEYS), low)

    @pl.when(c == 0)
    def _():
        for h in range(heads):
            if carried:
                mix_s[h] = st_in[0, h, : HEAD + 8, :]
                top_s[h : h + 1, :] = st_in[0, h, HEAD + 8 : HEAD + 9, :]
            else:
                top_s[h : h + 1, :] = jnp.full((1, cols), NEG, jnp.float32)
                mix_s[h] = jnp.zeros((HEAD + 8, cols), jnp.float32)

    def block(j, pieces, masked):
        here = pl.ds(pl.multiple_of(j * KEYS, KEYS), KEYS)
        scores = [_dot(k_ref[h, here, :], q_ref[h, at, :], 1, 1) for h, at in pieces]
        weights, keeps = [], []
        for (h, at), s in zip(pieces, scores):
            if masked:
                seen = lax.broadcasted_iota(jnp.int32, s.shape, 1) >= lax.broadcasted_iota(jnp.int32, s.shape, 0)
                s = jnp.where(seen, s, HIDDEN)
            old = top_s[h : h + 1, at]
            top = jnp.maximum(old, s.max(axis=0, keepdims=True))
            top_s[h : h + 1, at] = top
            weights.append(jnp.exp2((s - top) * e).astype(low))
            keeps.append(jnp.exp2((old - top) * e))
        for (h, at), p, keep in zip(pieces, weights, keeps):
            values = jnp.concatenate([vt_ref[h, :, here], ones], axis=0)
            mix_s[h, :, at] = mix_s[h, :, at] * keep + _dot(values, p, 1, 0)

    @pl.when(mode == 1)
    def _():
        every = [(h, pl.ds(n * STRIP, STRIP)) for h in range(heads) for n in range(strips)]
        lax.fori_loop(0, cols // KEYS, lambda j, _: block(j, every, False), None)

    @pl.when(mode == 2)
    def _():
        def strip(n, masked, j):
            at = pl.ds(pl.multiple_of(n * STRIP, STRIP), STRIP)
            block(j, [(h, at) for h in range(heads)], masked)

        def column(n, _):
            lax.fori_loop(0, n, lambda j, _: strip(n, False, j), None)
            strip(n, True, n)

        lax.fori_loop(0, strips, column, None)

    @pl.when(c == steps - 1)
    def _():
        for h in range(heads):
            total = mix_s[h, HEAD : HEAD + 1, :]
            o_ref[:, h * HEAD : (h + 1) * HEAD] = (mix_s[h, :HEAD, :] * (1 / total)).T.astype(low)
            if kept:
                st_out[0, h, : HEAD + 8, :] = mix_s[h]
                st_out[0, h, HEAD + 8 :, :] = jnp.broadcast_to(top_s[h : h + 1, :], (8, cols))


def attend(rows, keys, modes, bufs, state=None, keep=False):
    q, k, vt = bufs
    heads, chunk = q.shape[0], rows[1]
    rows = rows[0]
    n, steps = len(rows), len(keys[0])
    flat = [*rows, *[k for ks in keys for k in ks], *[m for ms in modes for m in ms]]
    tab = jnp.stack([jnp.asarray(t, jnp.int32) for t in flat])
    carried = state is not None
    at = lambda r, c, tab: tab[n + r * steps + c]
    in_specs = [
        pl.BlockSpec((heads, chunk, HEAD), lambda r, c, tab: (0, tab[r], 0)),
        pl.BlockSpec((heads, chunk, HEAD), lambda r, c, tab: (0, at(r, c, tab), 0)),
        pl.BlockSpec((heads, HEAD, chunk), lambda r, c, tab: (0, 0, at(r, c, tab))),
    ]
    st_spec = pl.BlockSpec((1, heads, HEAD + 16, chunk), lambda r, c, tab: (r, 0, 0, 0))
    given = [q, k, vt]
    if carried:
        given.append(state[0])
        in_specs.append(pl.BlockSpec((1, heads, HEAD + 16, chunk), lambda r, c, tab: (state[1], 0, 0, 0)))
    out_specs = [pl.BlockSpec((chunk, heads * HEAD), lambda r, c, tab: (r, 0))]
    out_shape = [jax.ShapeDtypeStruct((n * chunk, heads * HEAD), jnp.bfloat16)]
    if keep:
        out_specs.append(st_spec)
        out_shape.append(jax.ShapeDtypeStruct((n, heads, HEAD + 16, chunk), jnp.float32))
    return pl.pallas_call(
        functools.partial(_attend_kernel, scale=HEAD**-0.5, steps=steps, carried=carried, kept=keep),
        grid_spec=pltpu.PrefetchScalarGridSpec(
            num_scalar_prefetch=1,
            grid=(n, steps),
            in_specs=in_specs,
            out_specs=out_specs,
            scratch_shapes=[pltpu.VMEM((heads, chunk), jnp.float32), pltpu.VMEM((heads, HEAD + 8, chunk), jnp.float32)],
        ),
        out_shape=out_shape,
        compiler_params=pltpu.CompilerParams(dimension_semantics=("arbitrary", "arbitrary"), vmem_limit_bytes=VMEM),
        cost_estimate=pl.CostEstimate(
            flops=2 * n * steps * heads * chunk * chunk * HEAD, transcendentals=n * steps * heads * chunk * chunk // 2, bytes_accessed=2**24
        ),
        name="attend",
    )(tab, *given)


def _out_kernel(ids_ref, x_ref, *rest):
    o_refs, w_refs, y_ref = rest[:4], rest[4:8], rest[8]
    total = x_ref[...].astype(jnp.float32)
    acc = None
    for o_ref, w_ref in zip(o_refs, w_refs):
        part = _dot(o_ref[...], w_ref[...], 1, 0)
        acc = part if acc is None else acc + part
    y_ref[...] = (total + acc).astype(jnp.bfloat16)


def project(ids, x, parts, wo, half, halves, base):
    rows, depth = x.shape[0] // halves, x.shape[1]
    width = parts[0].shape[1]
    tiles = rows // ROWS
    specs = [pl.BlockSpec((ROWS, depth), lambda r, ids: (half * tiles + r, 0))]
    specs += [pl.BlockSpec((ROWS, width), lambda r, ids: (r, 0))] * 4
    specs += [pl.BlockSpec((width, depth), lambda r, ids, n=n: (ids[n], 0), pipeline_mode=pl.Buffered(1)) for n in range(4)]
    given = [x, *parts, *[wo] * 4]
    body, alias = _out_kernel, {}
    if base is not None:
        given.append(base)
        specs.append(pl.BlockSpec(memory_space=pl.ANY))
        alias = {10: 0}
        body = lambda *refs: _out_kernel(*refs[:10], refs[11])
    return pl.pallas_call(
        body,
        grid_spec=pltpu.PrefetchScalarGridSpec(
            num_scalar_prefetch=1,
            grid=(tiles,),
            in_specs=specs,
            out_specs=pl.BlockSpec((ROWS, depth), lambda r, ids: (half * tiles + r, 0)),
        ),
        out_shape=jax.ShapeDtypeStruct(x.shape, x.dtype),
        input_output_aliases=alias,
        compiler_params=pltpu.CompilerParams(dimension_semantics=("arbitrary",), vmem_limit_bytes=VMEM),
        cost_estimate=pl.CostEstimate(flops=2 * rows * 4 * width * depth, transcendentals=0, bytes_accessed=4 * rows * depth + 8 * width * depth),
        name="project",
    )(ids, *given)


def solution(mesh):
    n, groups = mesh.shape["sp"], mesh.shape["dp"]
    right = [(i, (i + 1) % n) for i in range(n)]
    left = [(i, (i - 1) % n) for i in range(n)]
    over = [(i, (i + 2) % n) for i in range(n)]
    pair = [(i, i ^ 1) for i in range(groups)]
    quad = [(i, i ^ 2) for i in range(groups)]

    def step(x, gain, wq, wk, wv, wo):
        own, depth = x.shape
        share = wq.shape[0]
        width = wq.shape[1] // n
        me, core = lax.axis_index("sp"), lax.axis_index("dp") % 2
        lft, rgt, opp = (me + n - 1) % n, (me + 1) % n, (me + 2) % n

        part = share // 2
        mine = jnp.stack([lax.dynamic_slice_in_dim(w, core * part, part, 0) for w in (wq, wk, wv)])

        def columns(ws, dev):
            cut = lax.dynamic_slice_in_dim(ws, dev * width, width, 2)
            return cut.transpose(1, 0, 2).reshape(ws.shape[1], 3 * width)

        with jax.named_scope("weights"):
            from_left = lax.ppermute(columns(mine, rgt), "sp", right)
            from_right = lax.ppermute(columns(mine, lft), "sp", left)
            from_opp = lax.ppermute(columns(mine, opp), "sp", over)
            got = jnp.stack([from_left, from_right, from_opp])
            other = lax.ppermute(got, "dp", pair)
        half = own // 2
        halves = [x[:half], x[half:]]
        with jax.named_scope("tokens"):
            l = [lax.ppermute(t, "sp", right) for t in halves]
            r = [lax.ppermute(t, "sp", left) for t in halves]
            o = [lax.ppermute(l[0], "sp", right), lax.ppermute(r[1], "sp", left)]

        w = jnp.zeros((n, 2, part, 3 * width), wq.dtype)
        place = lambda w, t, dev, c: lax.dynamic_update_slice(w, t[None, None], (dev, c, 0, 0))
        own_cols = columns(jnp.stack([wq, wk, wv]), me)
        w = lax.dynamic_update_slice(w, own_cols.reshape(1, 2, part, 3 * width), (me, 0, 0, 0))
        for i, dev in enumerate((lft, rgt, opp)):
            w = place(place(w, got[i], dev, core), other[i], dev, 1 - core)
        w = w.reshape(n * share, 3 * width)

        tokens = n * own
        angle = jnp.arange(tokens, dtype=jnp.float32)[:, None] * THETA ** (-jnp.arange(HEAD // 2, dtype=jnp.float32) / (HEAD // 2))
        cos, sin = jnp.cos(angle), jnp.sin(angle)
        gain2 = gain.reshape(1, depth)
        make = lambda first, t, bufs: qkv(first, t, gain2, w, cos, sin, bufs)
        bufs = make(me * own, x, [])
        for h in range(2):
            bufs = make(lft * own + h * half, l[h], bufs)
            bufs = make(rgt * own + h * half, r[h], bufs)
        mode = lambda row, key: jnp.where(key < row, 1, jnp.where(key == row, 2, 0))
        three = [rgt, lft, me]
        _, state = attend((three, own), [three] * 3, [[mode(i, j) for j in three] for i in three], bufs, keep=True)
        for h in range(2):
            bufs = make(opp * own + h * half, o[h], bufs)

        def finish(i):
            return attend(([three[i]], own), [[opp]], [[(opp < three[i]).astype(jnp.int32)]], bufs, state=(state, i))[0]

        to_right = finish(0)
        to_left = finish(1)
        every = [jnp.int32(j) for j in range(n)]
        to_opp = attend(([opp], own), [every], [[mode(opp, j) for j in every]], bufs)[0]
        mine_o = finish(2)

        with jax.named_scope("wo"):
            lot = lax.axis_index("dp") % 4
            bit = wo.shape[0] // 4
            wo_late, _ = lax.optimization_barrier((wo, l[0]))
            q4 = lax.dynamic_slice_in_dim(wo_late, lot * bit, bit, 0)
            a = jnp.stack([lax.ppermute(q4, "sp", right), lax.ppermute(q4, "sp", left), lax.ppermute(q4, "sp", over)])
            b = lax.ppermute(a, "dp", quad)
            ab = jnp.stack([a, b])
            cd = lax.ppermute(ab, "dp", pair)
            full = jnp.zeros((n, 4, bit, depth), wo.dtype)
            full = lax.dynamic_update_slice(full, wo.reshape(1, 4, bit, depth), (me, 0, 0, 0))
            for i, dev in enumerate((lft, rgt, opp)):
                for t, where in ((ab[0], lot), (ab[1], lot ^ 2), (cd[0], lot ^ 1), (cd[1], lot ^ 3)):
                    full = lax.dynamic_update_slice(full, t[i][None, None], (dev, where, 0, 0))
            full = full.reshape(n * share, depth)

        ids = jnp.stack([me, lft, rgt, opp]).astype(jnp.int32)
        cuts = 2
        y = None
        size = own // cuts
        with jax.named_scope("results"):
            for c in range(cuts):
                s = slice(c * size, (c + 1) * size)
                parts = [mine_o[s], lax.ppermute(to_right[s], "sp", right), lax.ppermute(to_left[s], "sp", left), lax.ppermute(to_opp[s], "sp", over)]
                y = project(ids, x, parts, full, c, cuts, y)
        return y

    tokens, whole = P(("dp", "sp"), None), P("sp", None)
    return jax.shard_map(
        step,
        mesh=mesh,
        in_specs=(tokens, P(None), whole, whole, whole, whole),
        out_specs=tokens,
        check_vma=False,
    )
```

```python
import functools

import jax
import jax.numpy as jnp
from jax import lax
from jax.experimental import pallas as pl
from jax.experimental.pallas import tpu as pltpu
from jax.sharding import PartitionSpec as P


HEAD = 256
THETA = 10000
NEG = -1e30
HIDDEN = 2 * NEG
LOG2E = 1.4426950408889634
VMEM = 56 * 2**20
STRIP = 512
KEYS = 512
CUT = 512
BLOCK = 1024
ROWS = 256


def _dot(a, b, ca, cb):
    return lax.dot_general(a, b, (((ca,), (cb,)), ((), ())), preferred_element_type=jnp.float32)


def normed(x, gain):
    wide = x.astype(jnp.float32)
    scale = lax.rsqrt(jnp.mean(wide * wide, -1, keepdims=True) + 1e-6)
    return (wide * scale * gain.astype(jnp.float32)).astype(jnp.bfloat16)


def _qkv_kernel(tab_ref, *refs, count, tiles):
    a_refs, (w_ref, cos_ref, sin_ref), (q_ref, k_ref, vt_ref) = refs[:count], refs[count : count + 3], refs[-3:]
    heads = q_ref.shape[0]
    half, width = HEAD // 2, heads * HEAD
    a = a_refs[0][...]
    for i in range(1, count):
        a = jnp.where(pl.program_id(0) < i * tiles, a, a_refs[i][...])
    cos, sin = cos_ref[...], sin_ref[...]
    for n, ref in enumerate((q_ref, k_ref)):
        t = _dot(a, w_ref[:, n * width : (n + 1) * width], 1, 0).astype(jnp.bfloat16).astype(jnp.float32)
        for h in range(heads):
            lo, hi = t[:, h * HEAD : h * HEAD + half], t[:, h * HEAD + half : (h + 1) * HEAD]
            ref[h, :, :half] = (lo * cos - hi * sin).astype(jnp.bfloat16)
            ref[h, :, half:] = (hi * cos + lo * sin).astype(jnp.bfloat16)
    v = _dot(a, w_ref[:, 2 * width :], 1, 0).astype(jnp.bfloat16)
    for h in range(heads):
        vt_ref[h] = v[:, h * HEAD : (h + 1) * HEAD].T


def qkv(firsts, xs, w, cos, sin, bufs):
    rows, depth = xs[0].shape
    heads = w.shape[1] // (3 * HEAD)
    shapes = [(heads, len(cos), HEAD), (heads, len(cos), HEAD), (heads, HEAD, len(cos))]
    tiles, count = rows // ROWS, len(xs)
    tab = jnp.stack([f // ROWS + t for f in firsts for t in range(tiles)]).astype(jnp.int32)
    table = pl.BlockSpec((ROWS, HEAD // 2), lambda r, tab: (tab[r], 0))
    anywhere = pl.BlockSpec(memory_space=pl.ANY)
    tokens = pl.BlockSpec((heads, ROWS, HEAD), lambda r, tab: (0, tab[r], 0))
    return pl.pallas_call(
        functools.partial(_qkv_kernel, count=count, tiles=tiles),
        grid_spec=pltpu.PrefetchScalarGridSpec(
            num_scalar_prefetch=1,
            grid=(tiles * count,),
            in_specs=[
                *[pl.BlockSpec((ROWS, depth), lambda r, tab, i=i: (jnp.clip(r - i * tiles, 0, tiles - 1), 0)) for i in range(count)],
                pl.BlockSpec(w.shape, lambda r, tab: (0, 0), pipeline_mode=pl.Buffered(1)),
                table,
                table,
                *[anywhere] * len(bufs),
            ],
            out_specs=[tokens, tokens, pl.BlockSpec((heads, HEAD, ROWS), lambda r, tab: (0, 0, tab[r]))],
        ),
        out_shape=[jax.ShapeDtypeStruct(s, w.dtype) for s in shapes],
        input_output_aliases={count + 4 + i: i for i in range(len(bufs))},
        compiler_params=pltpu.CompilerParams(dimension_semantics=("arbitrary",), vmem_limit_bytes=VMEM),
        cost_estimate=pl.CostEstimate(
            flops=2 * count * rows * depth * w.shape[1], transcendentals=0, bytes_accessed=2 * (count * rows * (depth + w.shape[1]) + w.size)
        ),
        name="qkv",
    )(tab, *xs, w, cos, sin, *bufs)


def _attend_kernel(tab_ref, q_ref, k_ref, vt_ref, *rest, scale, carried, final):
    st_in = rest[0] if carried else None
    outs, (top_s, mix_s) = rest[carried:-2], rest[-2:]
    heads, rows = q_ref.shape[0], q_ref.shape[1]
    _, _, mode, start, end = (tab_ref[i, pl.program_id(0)] for i in range(5))
    e = scale * LOG2E
    low = jnp.bfloat16

    def fresh():
        for h in range(heads):
            top_s[h : h + 1, :] = jnp.full((1, rows), NEG, jnp.float32)
            mix_s[h] = jnp.zeros((HEAD + 8, rows), jnp.float32)

    def resume():
        for h in range(heads):
            mix_s[h] = st_in[0, h, : HEAD + 8, :]
            top_s[h : h + 1, :] = st_in[0, h, HEAD + 8 : HEAD + 9, :]

    pl.when(start == 1)(fresh)
    if carried:
        pl.when(start == 2)(resume)

    def block(pieces):
        scores = [_dot(k_ref[h, lo : lo + keys, :], q_ref[h, at : at + STRIP, :], 1, 1) for h, at, lo, keys, _ in pieces]
        weights, keeps = [], []
        for (h, at, lo, _, masked), s in zip(pieces, scores):
            if masked:
                seen = lax.broadcasted_iota(jnp.int32, s.shape, 1) + (at - lo) >= lax.broadcasted_iota(jnp.int32, s.shape, 0)
                s = jnp.where(seen, s, HIDDEN)
            old = top_s[h : h + 1, at : at + STRIP]
            top = jnp.maximum(old, s.max(axis=0, keepdims=True))
            top_s[h : h + 1, at : at + STRIP] = top
            weights.append(jnp.exp2((s - top) * e).astype(low))
            keeps.append(jnp.exp2((old - top) * e))
        for (h, at, lo, keys, _), p, keep in zip(pieces, weights, keeps):
            values = jnp.concatenate([vt_ref[h, :, lo : lo + keys], jnp.ones((8, keys), low)], axis=0)
            mix_s[h, :, at : at + STRIP] = mix_s[h, :, at : at + STRIP] * keep + _dot(values, p, 1, 0)

    @pl.when(mode == 1)
    def _():
        for lo in range(0, rows, KEYS):
            block([(h, at, lo, KEYS, False) for h in range(heads) for at in range(0, rows, STRIP)])

    @pl.when(mode == 2)
    def _():
        for lo in range(0, rows, CUT):
            block([(h, at, lo, CUT, at < lo + CUT) for h in range(heads) for at in range(0, rows, STRIP) if at + STRIP > lo])

    @pl.when(end > 0)
    def _():
        for h in range(heads):
            if final:
                out = (mix_s[h, :HEAD, :] * (1 / mix_s[h, HEAD : HEAD + 1, :])).T.astype(low)
                for i, o_ref in enumerate(outs):

                    @pl.when(end == 1 + i)
                    def _():
                        o_ref[:, h * HEAD : (h + 1) * HEAD] = out

            else:
                outs[0][0, h, : HEAD + 8, :] = mix_s[h]
                outs[0][0, h, HEAD + 8 :, :] = jnp.broadcast_to(top_s[h : h + 1, :], (8, rows))


def _items(old, new, seen):
    items = []
    for n, i in enumerate([*old, *new]):
        keys = [j for j in seen[n >= len(old)] if j <= i]
        if not keys and n < len(old) and not seen[2]:
            continue
        mine = [[i, j, 2 if j == i else 1, 0, 0] for j in keys] or [[i, i, 0, 0, 0]]
        mine[0][3] = 2 if n < len(old) else 1
        mine[-1][4] = 1 + n
        items += mine
    return items


def attend(me, plans, bufs, state=None, final=False):
    q, k, vt = bufs
    heads, tokens = q.shape[0], q.shape[1]
    rows = BLOCK
    lists = [_items(old, new, (ko, kn, final)) for old, new, ko, kn in plans]
    steps = max(len(items) for items in lists)
    lists = [items + [items[-1][:2] + [0, 0, 0]] * (steps - len(items)) for items in lists]
    tab = lax.dynamic_index_in_dim(jnp.asarray(lists, jnp.int32).transpose(0, 2, 1), me, 0, False)
    carried = state is not None
    st_spec = pl.BlockSpec((1, heads, HEAD + 16, rows), lambda s, tab: (tab[0, s], 0, 0, 0))
    in_specs = [
        pl.BlockSpec((heads, rows, HEAD), lambda s, tab: (0, tab[0, s], 0)),
        pl.BlockSpec((heads, rows, HEAD), lambda s, tab: (0, tab[1, s], 0)),
        pl.BlockSpec((heads, HEAD, rows), lambda s, tab: (0, 0, tab[1, s])),
    ]
    given = [q, k, vt]
    if carried:
        given.append(state)
        in_specs.append(st_spec)
    if final:
        n = len(plans[0][0]) + len(plans[0][1])
        out_specs = [pl.BlockSpec((rows, heads * HEAD), lambda s, tab: (0, 0))] * n
        out_shape = [jax.ShapeDtypeStruct((rows, heads * HEAD), jnp.bfloat16)] * n
    else:
        out_specs = [st_spec]
        out_shape = [jax.ShapeDtypeStruct((tokens // rows, heads, HEAD + 16, rows), jnp.float32)]
    work = steps * heads * rows * rows
    got = pl.pallas_call(
        functools.partial(_attend_kernel, scale=HEAD**-0.5, carried=carried, final=final),
        grid_spec=pltpu.PrefetchScalarGridSpec(
            num_scalar_prefetch=1,
            grid=(steps,),
            in_specs=in_specs,
            out_specs=out_specs,
            scratch_shapes=[pltpu.VMEM((heads, rows), jnp.float32), pltpu.VMEM((heads, HEAD + 8, rows), jnp.float32)],
        ),
        out_shape=out_shape,
        input_output_aliases={4: 0} if carried and not final else {},
        compiler_params=pltpu.CompilerParams(dimension_semantics=("arbitrary",), vmem_limit_bytes=VMEM),
        cost_estimate=pl.CostEstimate(flops=4 * work * HEAD, transcendentals=work, bytes_accessed=2**24),
        name="attend",
    )(tab, *given)
    return got if final else got[0]


def _out_kernel(ids_ref, x_ref, *rest):
    o_refs, w_refs, y_ref = rest[:4], rest[4:8], rest[8]
    total = x_ref[...].astype(jnp.float32)
    acc = None
    for o_ref, w_ref in zip(o_refs, w_refs):
        part = _dot(o_ref[...], w_ref[...], 1, 0)
        acc = part if acc is None else acc + part
    y_ref[...] = (total + acc).astype(jnp.bfloat16)


def project(ids, x, parts, wo, half, halves, base):
    rows, depth = x.shape[0] // halves, x.shape[1]
    width = parts[0].shape[1]
    tiles = rows // ROWS
    specs = [pl.BlockSpec((ROWS, depth), lambda r, ids: (half * tiles + r, 0))]
    specs += [pl.BlockSpec((ROWS, width), lambda r, ids: (r, 0))] * 4
    specs += [pl.BlockSpec((width, depth), lambda r, ids, n=n: (ids[n], 0), pipeline_mode=pl.Buffered(1)) for n in range(4)]
    given = [x, *parts, *[wo] * 4]
    body, alias = _out_kernel, {}
    if base is not None:
        given.append(base)
        specs.append(pl.BlockSpec(memory_space=pl.ANY))
        alias = {10: 0}
        body = lambda *refs: _out_kernel(*refs[:10], refs[11])
    return pl.pallas_call(
        body,
        grid_spec=pltpu.PrefetchScalarGridSpec(
            num_scalar_prefetch=1,
            grid=(tiles,),
            in_specs=specs,
            out_specs=pl.BlockSpec((ROWS, depth), lambda r, ids: (half * tiles + r, 0)),
        ),
        out_shape=jax.ShapeDtypeStruct(x.shape, x.dtype),
        input_output_aliases=alias,
        compiler_params=pltpu.CompilerParams(dimension_semantics=("arbitrary",), vmem_limit_bytes=VMEM),
        cost_estimate=pl.CostEstimate(flops=2 * rows * 4 * width * depth, transcendentals=0, bytes_accessed=4 * rows * depth + 8 * width * depth),
        name="project",
    )(ids, *given)


def _place_kernel(tab_ref, *refs, owned):
    out_ref, at = refs[-1], owned[1]
    columns = out_ref.shape[2] // owned[0]
    for j, ref in enumerate(refs[: owned[0]]):
        rows = ref.shape[0] // owned[1]
        for i in range(owned[1]):
            out_ref[tab_ref[i], :, j * columns : (j + 1) * columns] = ref[i * rows : (i + 1) * rows, :]
    for ref in refs[owned[0] : -1]:
        for i in range(ref.shape[0]):
            out_ref[tab_ref[at]] = ref[i]
            at += 1


def place(slots, own, arrays):
    count, rows, columns = len(slots), *arrays[0].shape[1:]
    tab = jnp.stack([jnp.asarray(s, jnp.int32) for s in [*slots, own[0][1]]])
    owned = (len(own), count - sum(len(t) for t in arrays))
    whole = lambda t: pl.BlockSpec(t.shape, lambda i, tab: (0,) * t.ndim)
    out = jax.ShapeDtypeStruct((count, rows, columns), arrays[0].dtype)
    return pl.pallas_call(
        functools.partial(_place_kernel, owned=owned),
        grid_spec=pltpu.PrefetchScalarGridSpec(
            num_scalar_prefetch=1,
            grid=(1,),
            in_specs=[
                *[pl.BlockSpec((w.shape[0], columns // len(own)), lambda i, tab: (0, tab[count])) for w, _ in own],
                *[whole(t) for t in arrays],
            ],
            out_specs=whole(out),
        ),
        out_shape=out,
        compiler_params=pltpu.CompilerParams(vmem_limit_bytes=VMEM),
        cost_estimate=pl.CostEstimate(flops=2**24, transcendentals=0, bytes_accessed=4 * count * rows * columns),
        name="place",
    )(tab, *[w for w, _ in own], *arrays).reshape(count * rows, columns)


def solution(mesh):
    n, groups = mesh.shape["sp"], mesh.shape["dp"]
    right = [(i, (i + 1) % n) for i in range(n)]
    left = [(i, (i - 1) % n) for i in range(n)]
    over = [(i, (i + 2) % n) for i in range(n)]
    pair = [(i, i ^ 1) for i in range(groups)]
    quad = [(i, i ^ 2) for i in range(groups)]

    def step(x, gain, wq, wk, wv, wo):
        own, _ = x.shape
        share = wq.shape[0]
        width = wq.shape[1] // n
        me, lot = lax.axis_index("sp"), lax.axis_index("dp") % 4
        lft, rgt, opp = (me + n - 1) % n, (me + 1) % n, (me + 2) % n
        bit = share // 4

        def gathered(t, cut):
            ways = ((rgt, right), (lft, left), (opp, over))
            a = jnp.stack([lax.ppermute(cut(t, d), "sp", p) for d, p in ways])
            b = lax.ppermute(a, "dp", quad)
            cd = lax.ppermute(jnp.concatenate([a, b]), "dp", pair)
            return [a, b, cd]

        slots = [me * 4 + i for i in range(4)]
        slots += [d * 4 + c for c in (lot, lot ^ 2, lot ^ 1, lot ^ 3) for d in (lft, rgt, opp)]

        def columns(ws, dev):
            cut = lax.dynamic_slice_in_dim(ws, dev * width, width, 2)
            return cut.transpose(1, 0, 2).reshape(ws.shape[1], 3 * width)

        mine = jnp.stack([lax.dynamic_slice_in_dim(w, lot * bit, bit, 0) for w in (wq, wk, wv)])
        parts = gathered(mine, columns)
        w = place(slots, [(wq, me), (wk, me), (wv, me)], parts)

        piece = own // 4
        a = [normed(x[i * piece : (i + 1) * piece], gain) for i in range(4)]
        l, r, o = [None] * 4, [None] * 4, [None] * 4
        for way in (0, 2):
            l[way], r[way + 1] = lax.ppermute(a[way], "sp", right), lax.ppermute(a[way + 1], "sp", left)
            l[way + 1], r[way] = lax.ppermute(a[way + 1], "sp", right), lax.ppermute(a[way], "sp", left)
            o[way], o[way + 1] = lax.ppermute(l[way], "sp", right), lax.ppermute(r[way + 1], "sp", left)

        tokens = n * own
        rate = THETA ** (-jnp.arange(HEAD // 2, dtype=jnp.float32) / (HEAD // 2))
        big = jnp.arange(0, tokens, 128, dtype=jnp.float32)[:, None, None] * rate
        small = jnp.arange(128, dtype=jnp.float32)[None, :, None] * rate
        cb, sb, cs, ss = lax.optimization_barrier((jnp.cos(big), jnp.sin(big), jnp.cos(small), jnp.sin(small)))
        cos, sin = (cb * cs - sb * ss).reshape(tokens, -1), (sb * cs + cb * ss).reshape(tokens, -1)

        def make(*pieces, bufs):
            return qkv([d * own + i * piece for d, _, i in pieces], [t[i] for _, t, i in pieces], w, cos, sin, bufs)

        ring = [[[2 * d, 2 * d + 1] for d in (m, (m - 1) % n, (m + 1) % n, (m + 2) % n)] for m in range(n)]
        plan = lambda f: [f(*blocks) for blocks in ring]
        bufs = make(*[(me, a, i) for i in range(4)], bufs=[])
        state = attend(me, plan(lambda o, l, r, c: ([], o, [], o)), bufs)
        bufs = make((lft, l, 0), (lft, l, 1), (rgt, r, 0), (rgt, r, 1), bufs=bufs)
        state = attend(me, plan(lambda o, l, r, c: (o, [l[0], r[0]], [l[0], r[0]], [*o, l[0], r[0]])), bufs, state)
        bufs = make((opp, o, 0), (opp, o, 1), bufs=bufs)
        state = attend(me, plan(lambda o, l, r, c: ([*o, l[0], r[0]], [c[0]], [c[0]], [*o, l[0], r[0], c[0]])), bufs, state)
        bufs = make((lft, l, 2), (rgt, r, 3), bufs=bufs)
        bufs = make((lft, l, 3), (rgt, r, 2), bufs=bufs)
        state = attend(me, plan(lambda o, l, r, c: ([*o, l[0], r[0], c[0]], [l[1], r[1]], [l[1], r[1]], [*o, *l, *r, c[0]])), bufs, state)
        bufs = make((opp, o, 2), (opp, o, 3), bufs=bufs)
        sides = attend(me, plan(lambda o, l, r, c: ([*r, *l], [], [c[1]], [])), bufs, state, True)
        to_right, to_left = sides[:2], sides[2:]
        to_opp = attend(me, plan(lambda o, l, r, c: ([c[0]], [c[1]], [], [*o, *l, *r, *c])), bufs, state, True)
        kept = attend(me, plan(lambda o, l, r, c: (o, [], [c[1]], [])), bufs, state, True)

        parts = gathered(lax.dynamic_slice_in_dim(wo, lot * bit, bit, 0), lambda t, d: t)
        full = place(slots, [(wo, 0)], parts)

        ids = jnp.stack([me, lft, rgt, opp]).astype(jnp.int32)
        y = None
        for c in range(2):
            parts = [lax.ppermute(t[c], "sp", p) for t, p in ((to_right, right), (to_left, left), (to_opp, over))]
            y = project(ids, x, [kept[c], *parts], full, c, 2, y)
        return y

    tokens, whole = P(("dp", "sp"), None), P("sp", None)
    return jax.shard_map(
        step,
        mesh=mesh,
        in_specs=(tokens, P(None), whole, whole, whole, whole),
        out_specs=tokens,
        check_vma=False,
    )
```

```python
import functools

import jax
import jax.numpy as jnp
from jax import lax
from jax.experimental import pallas as pl
from jax.experimental.pallas import tpu as pltpu
from jax.sharding import PartitionSpec as P


HEAD = 256
THETA = 10000
NEG = -1e30
HIDDEN = 2 * NEG
LOG2E = 1.4426950408889634
VMEM = 56 * 2**20
STRIP = 512
KEYS = 512
CUT = 512
BLOCK = 1024
ROWS = 256


def _dot(a, b, ca, cb):
    return lax.dot_general(a, b, (((ca,), (cb,)), ((), ())), preferred_element_type=jnp.float32)


def normed(x, gain):
    wide = x.astype(jnp.float32)
    scale = lax.rsqrt(jnp.mean(wide * wide, -1, keepdims=True) + 1e-6)
    return (wide * scale * gain.astype(jnp.float32)).astype(jnp.bfloat16)


def _qkv_kernel(tab_ref, *refs, count, tiles):
    a_refs, (w_ref, cos_ref, sin_ref), (q_ref, k_ref, vt_ref) = refs[:count], refs[count : count + 3], refs[-3:]
    heads = q_ref.shape[0]
    half, width = HEAD // 2, heads * HEAD
    a = a_refs[0][...]
    for i in range(1, count):
        a = jnp.where(pl.program_id(0) < i * tiles, a, a_refs[i][...])
    cos, sin = cos_ref[...], sin_ref[...]
    for n, ref in enumerate((q_ref, k_ref)):
        t = _dot(a, w_ref[:, n * width : (n + 1) * width], 1, 0).astype(jnp.bfloat16).astype(jnp.float32)
        for h in range(heads):
            lo, hi = t[:, h * HEAD : h * HEAD + half], t[:, h * HEAD + half : (h + 1) * HEAD]
            ref[h, :, :half] = (lo * cos - hi * sin).astype(jnp.bfloat16)
            ref[h, :, half:] = (hi * cos + lo * sin).astype(jnp.bfloat16)
    v = _dot(a, w_ref[:, 2 * width :], 1, 0).astype(jnp.bfloat16)
    for h in range(heads):
        vt_ref[h] = v[:, h * HEAD : (h + 1) * HEAD].T


def qkv(firsts, xs, w, cos, sin, bufs):
    rows, depth = xs[0].shape
    heads = w.shape[1] // (3 * HEAD)
    shapes = [(heads, len(cos), HEAD), (heads, len(cos), HEAD), (heads, HEAD, len(cos))]
    tiles, count = rows // ROWS, len(xs)
    tab = jnp.stack([f // ROWS + t for f in firsts for t in range(tiles)]).astype(jnp.int32)
    table = pl.BlockSpec((ROWS, HEAD // 2), lambda r, tab: (tab[r], 0))
    anywhere = pl.BlockSpec(memory_space=pl.ANY)
    tokens = pl.BlockSpec((heads, ROWS, HEAD), lambda r, tab: (0, tab[r], 0))
    return pl.pallas_call(
        functools.partial(_qkv_kernel, count=count, tiles=tiles),
        grid_spec=pltpu.PrefetchScalarGridSpec(
            num_scalar_prefetch=1,
            grid=(tiles * count,),
            in_specs=[
                *[pl.BlockSpec((ROWS, depth), lambda r, tab, i=i: (jnp.clip(r - i * tiles, 0, tiles - 1), 0)) for i in range(count)],
                pl.BlockSpec(w.shape, lambda r, tab: (0, 0), pipeline_mode=pl.Buffered(1)),
                table,
                table,
                *[anywhere] * len(bufs),
            ],
            out_specs=[tokens, tokens, pl.BlockSpec((heads, HEAD, ROWS), lambda r, tab: (0, 0, tab[r]))],
        ),
        out_shape=[jax.ShapeDtypeStruct(s, w.dtype) for s in shapes],
        input_output_aliases={count + 4 + i: i for i in range(len(bufs))},
        compiler_params=pltpu.CompilerParams(dimension_semantics=("arbitrary",), vmem_limit_bytes=VMEM),
        cost_estimate=pl.CostEstimate(
            flops=2 * count * rows * depth * w.shape[1], transcendentals=0, bytes_accessed=2 * (count * rows * (depth + w.shape[1]) + w.size)
        ),
        name="qkv",
    )(tab, *xs, w, cos, sin, *bufs)


def _attend_kernel(tab_ref, q_ref, k_ref, vt_ref, *rest, scale, carried, keep, modes):
    st_in = rest[0] if carried else None
    outs, (top_s, mix_s) = rest[carried:-2], rest[-2:]
    heads, rows = q_ref.shape[0], q_ref.shape[1]
    _, _, mode, start, end = (tab_ref[i, pl.program_id(0)] for i in range(5))
    e = scale * LOG2E
    low = jnp.bfloat16

    def fresh():
        for h in range(heads):
            top_s[h : h + 1, :] = jnp.full((1, rows), NEG, jnp.float32)
            mix_s[h] = jnp.zeros((HEAD + 8, rows), jnp.float32)

    def resume():
        for h in range(heads):
            mix_s[h] = st_in[0, h, : HEAD + 8, :]
            top_s[h : h + 1, :] = st_in[0, h, HEAD + 8 : HEAD + 9, :]

    pl.when(start == 1)(fresh)
    if carried:
        pl.when(start == 2)(resume)

    def block(pieces):
        scores = [_dot(k_ref[h, lo : lo + keys, :], q_ref[h, at : at + STRIP, :], 1, 1) for h, at, lo, keys, _ in pieces]
        weights, keeps = [], []
        for (h, at, lo, _, masked), s in zip(pieces, scores):
            if masked:
                seen = lax.broadcasted_iota(jnp.int32, s.shape, 1) + (at - lo) >= lax.broadcasted_iota(jnp.int32, s.shape, 0)
                s = jnp.where(seen, s, HIDDEN)
            old = top_s[h : h + 1, at : at + STRIP]
            top = jnp.maximum(old, s.max(axis=0, keepdims=True))
            top_s[h : h + 1, at : at + STRIP] = top
            weights.append(jnp.exp2((s - top) * e).astype(low))
            keeps.append(jnp.exp2((old - top) * e))
        for (h, at, lo, keys, _), p, keep in zip(pieces, weights, keeps):
            values = jnp.concatenate([vt_ref[h, :, lo : lo + keys], jnp.ones((8, keys), low)], axis=0)
            mix_s[h, :, at : at + STRIP] = mix_s[h, :, at : at + STRIP] * keep + _dot(values, p, 1, 0)

    def whole():
        for lo in range(0, rows, KEYS):
            block([(h, at, lo, KEYS, False) for h in range(heads) for at in range(0, rows, STRIP)])

    def cut():
        for lo in range(0, rows, CUT):
            block([(h, at, lo, CUT, at < lo + CUT) for h in range(heads) for at in range(0, rows, STRIP) if at + STRIP > lo])

    if 1 in modes:
        pl.when(mode == 1)(whole)
    if 2 in modes:
        pl.when(mode == 2)(cut)

    if keep:

        @pl.when(end == 1)
        def _():
            for h in range(heads):
                outs[0][0, h, : HEAD + 8, :] = mix_s[h]
                outs[0][0, h, HEAD + 8 :, :] = jnp.broadcast_to(top_s[h : h + 1, :], (8, rows))

    for i, o_ref in enumerate(outs[keep:]):

        @pl.when(end == 2 + i)
        def _():
            for h in range(heads):
                out = (mix_s[h, :HEAD, :] * (1 / mix_s[h, HEAD : HEAD + 1, :])).T
                o_ref[:, h * HEAD : (h + 1) * HEAD] = out.astype(low)


def _items(rows, finals):
    items = []
    for i, keys, fresh in rows:
        keys = [j for j in keys if j <= i]
        if not keys and i not in finals:
            continue
        mine = [[i, j, 2 if j == i else 1, 0, 0] for j in keys] or [[i, i, 0, 0, 0]]
        mine[0][3] = 1 if fresh else 2
        mine[-1][4] = 2 + finals.index(i) if i in finals else 1
        items += mine
    return items


def attend(me, plans, bufs, state=None, keep=True):
    q, k, vt = bufs
    heads, tokens = q.shape[0], q.shape[1]
    rows = BLOCK
    lists = [_items(*p) for p in plans]
    modes = {item[2] for items in lists for item in items}
    steps = max(len(items) for items in lists)
    lists = [items + [items[-1][:2] + [0, 0, 0]] * (steps - len(items)) for items in lists]
    tab = lax.dynamic_index_in_dim(jnp.asarray(lists, jnp.int32).transpose(0, 2, 1), me, 0, False)
    carried = state is not None
    st_spec = pl.BlockSpec((1, heads, HEAD + 16, rows), lambda s, tab: (tab[0, s], 0, 0, 0))
    in_specs = [
        pl.BlockSpec((heads, rows, HEAD), lambda s, tab: (0, tab[0, s], 0)),
        pl.BlockSpec((heads, rows, HEAD), lambda s, tab: (0, tab[1, s], 0)),
        pl.BlockSpec((heads, HEAD, rows), lambda s, tab: (0, 0, tab[1, s])),
    ]
    given = [q, k, vt]
    if carried:
        given.append(state)
        in_specs.append(st_spec)
    n = len(plans[0][1])
    out_specs = [st_spec] * keep + [pl.BlockSpec((rows, heads * HEAD), lambda s, tab: (0, 0))] * n
    out_shape = [jax.ShapeDtypeStruct((tokens // rows, heads, HEAD + 16, rows), jnp.float32)] * keep
    out_shape += [jax.ShapeDtypeStruct((rows, heads * HEAD), jnp.bfloat16)] * n
    work = steps * heads * rows * rows
    return pl.pallas_call(
        functools.partial(_attend_kernel, scale=HEAD**-0.5, carried=carried, keep=keep, modes=modes),
        grid_spec=pltpu.PrefetchScalarGridSpec(
            num_scalar_prefetch=1,
            grid=(steps,),
            in_specs=in_specs,
            out_specs=out_specs,
            scratch_shapes=[pltpu.VMEM((heads, rows), jnp.float32), pltpu.VMEM((heads, HEAD + 8, rows), jnp.float32)],
        ),
        out_shape=out_shape,
        input_output_aliases={4: 0} if carried and keep else {},
        compiler_params=pltpu.CompilerParams(dimension_semantics=("arbitrary",), vmem_limit_bytes=VMEM),
        cost_estimate=pl.CostEstimate(flops=4 * work * HEAD, transcendentals=work, bytes_accessed=2**24),
        name="attend",
    )(tab, *given)


def _out_kernel(ids_ref, *refs, count, first):
    base, o_refs, w_refs = refs[0], refs[first : first + count], refs[first + count : first + 2 * count]
    y_ref = refs[-1]
    acc = None
    for o_ref, w_ref in zip(o_refs, w_refs):
        part = _dot(o_ref[...], w_ref[...], 1, 0)
        acc = part if acc is None else acc + part
    if first == 2:
        acc = refs[1][...] + acc
    if first:
        acc = base[...].astype(jnp.float32) + acc
    y_ref[...] = acc.astype(y_ref.dtype)


def project(ids, parts, wo, rest=None):
    (rows, width), depth, count = parts[0].shape, wo.shape[1], len(parts)
    tiles = rows // ROWS
    given = [*parts, *[wo] * count]
    specs = [pl.BlockSpec((ROWS, width), lambda r, ids: (r, 0))] * count
    specs += [pl.BlockSpec((width, depth), lambda r, ids, n=n: (ids[n], 0), pipeline_mode=pl.Buffered(1)) for n in range(count)]
    out, at, alias, first = jax.ShapeDtypeStruct((rows, depth), jnp.float32), lambda r, ids: (r, 0), {}, 0
    if rest is not None:
        x, total, half, y = rest
        at, before = lambda r, ids: (half * tiles + r, 0), [x] if total is None else [x, total]
        first = len(before)
        given = [*before, *given]
        specs = [pl.BlockSpec((ROWS, depth), at), pl.BlockSpec((ROWS, depth), lambda r, ids: (r, 0))][:first] + specs
        out = jax.ShapeDtypeStruct(x.shape, x.dtype)
        if y is not None:
            alias = {1 + len(given): 0}
            given.append(y)
            specs.append(pl.BlockSpec(memory_space=pl.ANY))
    return pl.pallas_call(
        functools.partial(_out_kernel, count=count, first=first),
        grid_spec=pltpu.PrefetchScalarGridSpec(
            num_scalar_prefetch=1, grid=(tiles,), in_specs=specs, out_specs=pl.BlockSpec((ROWS, depth), at)
        ),
        out_shape=out,
        input_output_aliases=alias,
        compiler_params=pltpu.CompilerParams(dimension_semantics=("arbitrary",), vmem_limit_bytes=VMEM),
        cost_estimate=pl.CostEstimate(
            flops=2 * rows * count * width * depth, transcendentals=0, bytes_accessed=4 * rows * depth + 2 * count * width * depth
        ),
        name="project",
    )(ids, *given)


def _place_kernel(tab_ref, *refs, owned):
    out_ref, at = refs[-1], owned[1]
    columns = out_ref.shape[2] // owned[0]
    for j, ref in enumerate(refs[: owned[0]]):
        rows = ref.shape[0] // owned[1]
        for i in range(owned[1]):
            out_ref[tab_ref[i], :, j * columns : (j + 1) * columns] = ref[i * rows : (i + 1) * rows, :]
    for ref in refs[owned[0] : -1]:
        for i in range(ref.shape[0]):
            out_ref[tab_ref[at]] = ref[i]
            at += 1


def place(slots, own, arrays):
    count, rows, columns = len(slots), *arrays[0].shape[1:]
    tab = jnp.stack([jnp.asarray(s, jnp.int32) for s in [*slots, own[0][1]]])
    owned = (len(own), count - sum(len(t) for t in arrays))
    whole = lambda t: pl.BlockSpec(t.shape, lambda i, tab: (0,) * t.ndim)
    out = jax.ShapeDtypeStruct((count, rows, columns), arrays[0].dtype)
    return pl.pallas_call(
        functools.partial(_place_kernel, owned=owned),
        grid_spec=pltpu.PrefetchScalarGridSpec(
            num_scalar_prefetch=1,
            grid=(1,),
            in_specs=[
                *[pl.BlockSpec((w.shape[0], columns // len(own)), lambda i, tab: (0, tab[count])) for w, _ in own],
                *[whole(t) for t in arrays],
            ],
            out_specs=whole(out),
        ),
        out_shape=out,
        compiler_params=pltpu.CompilerParams(vmem_limit_bytes=VMEM),
        cost_estimate=pl.CostEstimate(flops=2**24, transcendentals=0, bytes_accessed=4 * count * rows * columns),
        name="place",
    )(tab, *[w for w, _ in own], *arrays).reshape(count * rows, columns)


def solution(mesh):
    n, groups = mesh.shape["sp"], mesh.shape["dp"]
    right = [(i, (i + 1) % n) for i in range(n)]
    left = [(i, (i - 1) % n) for i in range(n)]
    over = [(i, (i + 2) % n) for i in range(n)]
    pair = [(i, i ^ 1) for i in range(groups)]
    quad = [(i, i ^ 2) for i in range(groups)]

    def step(x, gain, wq, wk, wv, wo):
        own, _ = x.shape
        share = wq.shape[0]
        width = wq.shape[1] // n
        me, lot = lax.axis_index("sp"), lax.axis_index("dp") % 4
        lft, rgt, opp = (me + n - 1) % n, (me + 1) % n, (me + 2) % n
        bit = share // 4

        def gathered(t, cut):
            ways = ((rgt, right), (lft, left), (opp, over))
            a = jnp.stack([lax.ppermute(cut(t, d), "sp", p) for d, p in ways])
            b = lax.ppermute(a, "dp", quad)
            cd = lax.ppermute(jnp.concatenate([a, b]), "dp", pair)
            return [a, b, cd]

        slots = [me * 4 + i for i in range(4)]
        slots += [d * 4 + c for c in (lot, lot ^ 2, lot ^ 1, lot ^ 3) for d in (lft, rgt, opp)]

        def columns(ws, dev):
            cut = lax.dynamic_slice_in_dim(ws, dev * width, width, 2)
            return cut.transpose(1, 0, 2).reshape(ws.shape[1], 3 * width)

        mine = jnp.stack([lax.dynamic_slice_in_dim(w, lot * bit, bit, 0) for w in (wq, wk, wv)])
        parts = gathered(mine, columns)
        w = place(slots, [(wq, me), (wk, me), (wv, me)], parts)

        piece = own // 4
        a = [normed(x[i * piece : (i + 1) * piece], gain) for i in range(4)]
        l, r, o = [None] * 4, [None] * 4, [None] * 4
        for way in (0, 2):
            l[way], r[way + 1] = lax.ppermute(a[way], "sp", right), lax.ppermute(a[way + 1], "sp", left)
            l[way + 1], r[way] = lax.ppermute(a[way + 1], "sp", right), lax.ppermute(a[way], "sp", left)
            o[way], o[way + 1] = lax.ppermute(l[way], "sp", right), lax.ppermute(r[way + 1], "sp", left)

        tokens = n * own
        rate = THETA ** (-jnp.arange(HEAD // 2, dtype=jnp.float32) / (HEAD // 2))
        big = jnp.arange(0, tokens, 128, dtype=jnp.float32)[:, None, None] * rate
        small = jnp.arange(128, dtype=jnp.float32)[None, :, None] * rate
        cb, sb, cs, ss = lax.optimization_barrier((jnp.cos(big), jnp.sin(big), jnp.cos(small), jnp.sin(small)))
        cos, sin = (cb * cs - sb * ss).reshape(tokens, -1), (sb * cs + cb * ss).reshape(tokens, -1)

        def make(*pieces, bufs):
            return qkv([d * own + i * piece for d, _, i in pieces], [t[i] for _, t, i in pieces], w, cos, sin, bufs)

        ring = [[[2 * d, 2 * d + 1] for d in (m, (m - 1) % n, (m + 1) % n, (m + 2) % n)] for m in range(n)]
        old = lambda rows, keys: [(i, keys, False) for i in rows]
        new = lambda rows, keys: [(i, keys, True) for i in rows]
        plan = lambda f: [f(*blocks) for blocks in ring]
        bufs = make(*[(me, a, i) for i in range(4)], bufs=[])
        (state,) = attend(me, plan(lambda o, l, r, c: (new(o, o), [])), bufs)
        bufs = make((lft, l, 0), (lft, l, 1), (rgt, r, 0), (rgt, r, 1), bufs=bufs)
        (state,) = attend(me, plan(lambda o, l, r, c: (old(o, [l[0], r[0]]) + new([l[0], r[0]], [*o, l[0], r[0]]), [])), bufs, state)
        bufs = make((opp, o, 0), (opp, o, 1), bufs=bufs)
        (state,) = attend(me, plan(lambda o, l, r, c: (old([*o, l[0], r[0]], [c[0]]) + new([c[0]], [*o, l[0], r[0], c[0]]), [])), bufs, state)
        bufs = make((lft, l, 2), (rgt, r, 3), bufs=bufs)
        bufs = make((lft, l, 3), (rgt, r, 2), bufs=bufs)
        last = plan(lambda o, l, r, c: (old([c[0], *o, l[0], r[0]], [l[1], r[1]]) + new([l[1], r[1]], [*o, *l, *r, c[0]]), [c[0]]))
        state, first_opp = attend(me, last, bufs, state)
        bufs = make((opp, o, 2), (opp, o, 3), bufs=bufs)

        def spread(call, o, l, r, c):
            keys = [j for j in range(c[1] + 1)]
            cuts = {0: (0, 0), 1: (1, 2), 2: (1, 2), 3: (2, 4)}[c[0] // 2]
            if call == 2:
                rows = old(o, [c[1]]) + [(c[1], keys[cuts[1] :], cuts[1] == 0)]
                return rows, [*o, c[1]]
            rows = old([r[call], l[call]], [c[1]])
            now = keys[cuts[0] : cuts[1]] if call else keys[: cuts[0]]
            return rows + [(c[1], now, call == 0)], [r[call], l[call]]

        sides = []
        for h in range(2):
            state, *got = attend(me, plan(functools.partial(spread, h)), bufs, state)
            sides.append(got)
        rest = attend(me, plan(functools.partial(spread, 2)), bufs, state, False)
        to_opp, kept = [first_opp, rest[2]], rest[:2]

        parts = gathered(lax.dynamic_slice_in_dim(wo, lot * bit, bit, 0), lambda t, d: t)
        full = place(slots, [(wo, 0)], parts)

        ids, far = jnp.stack([me, lft, rgt]).astype(jnp.int32), opp.astype(jnp.int32).reshape(1)
        near, sent = [], []
        for h in range(2):
            near.append([kept[h], lax.ppermute(sides[h][0], "sp", right), lax.ppermute(sides[h][1], "sp", left)])
        for h in range(2):
            sent.append(lax.ppermute(to_opp[h], "sp", over))
        y = project(jnp.concatenate([ids, far]), [*near[0], sent[0]], full, (x, None, 0, None))
        y = project(jnp.concatenate([ids, far]), [*near[1], sent[1]], full, (x, None, 1, y))
        return y

    tokens, whole = P(("dp", "sp"), None), P("sp", None)
    return jax.shard_map(
        step,
        mesh=mesh,
        in_specs=(tokens, P(None), whole, whole, whole, whole),
        out_specs=tokens,
        check_vma=False,
    )
```

```python
import functools

import jax
import jax.numpy as jnp
from jax import lax
from jax.experimental import pallas as pl
from jax.experimental.pallas import tpu as pltpu
from jax.sharding import PartitionSpec as P


HEAD = 256
THETA = 10000
NEG = -1e30
HIDDEN = 2 * NEG
LOG2E = 1.4426950408889634
VMEM = 56 * 2**20
STRIP = 512
KEYS = 512
CUT = 512
BLOCK = 1024
ROWS = 256


def _dot(a, b, ca, cb):
    return lax.dot_general(a, b, (((ca,), (cb,)), ((), ())), preferred_element_type=jnp.float32)


def normed(x, gain):
    wide = x.astype(jnp.float32)
    scale = lax.rsqrt(jnp.mean(wide * wide, -1, keepdims=True) + 1e-6)
    return (wide * scale * gain.astype(jnp.float32)).astype(jnp.bfloat16)


def _qkv_kernel(tab_ref, *refs, count, tiles):
    a_refs, (w_ref, cos_ref, sin_ref), (q_ref, k_ref, vt_ref) = refs[:count], refs[count : count + 3], refs[-3:]
    heads = q_ref.shape[0]
    half, width = HEAD // 2, heads * HEAD
    a = a_refs[0][...]
    for i in range(1, count):
        a = jnp.where(pl.program_id(0) < i * tiles, a, a_refs[i][...])
    cos, sin = cos_ref[...], sin_ref[...]
    for n, ref in enumerate((q_ref, k_ref)):
        t = _dot(a, w_ref[:, n * width : (n + 1) * width], 1, 0).astype(jnp.bfloat16).astype(jnp.float32)
        for h in range(heads):
            lo, hi = t[:, h * HEAD : h * HEAD + half], t[:, h * HEAD + half : (h + 1) * HEAD]
            ref[h, :, :half] = (lo * cos - hi * sin).astype(jnp.bfloat16)
            ref[h, :, half:] = (hi * cos + lo * sin).astype(jnp.bfloat16)
    v = _dot(a, w_ref[:, 2 * width :], 1, 0).astype(jnp.bfloat16)
    for h in range(heads):
        vt_ref[h] = v[:, h * HEAD : (h + 1) * HEAD].T


def qkv(firsts, xs, w, cos, sin, bufs):
    rows, depth = xs[0].shape
    heads = w.shape[1] // (3 * HEAD)
    shapes = [(heads, len(cos), HEAD), (heads, len(cos), HEAD), (heads, HEAD, len(cos))]
    tiles, count = rows // ROWS, len(xs)
    tab = jnp.stack([f // ROWS + t for f in firsts for t in range(tiles)]).astype(jnp.int32)
    table = pl.BlockSpec((ROWS, HEAD // 2), lambda r, tab: (tab[r], 0))
    anywhere = pl.BlockSpec(memory_space=pl.ANY)
    tokens = pl.BlockSpec((heads, ROWS, HEAD), lambda r, tab: (0, tab[r], 0))
    return pl.pallas_call(
        functools.partial(_qkv_kernel, count=count, tiles=tiles),
        grid_spec=pltpu.PrefetchScalarGridSpec(
            num_scalar_prefetch=1,
            grid=(tiles * count,),
            in_specs=[
                *[pl.BlockSpec((ROWS, depth), lambda r, tab, i=i: (jnp.clip(r - i * tiles, 0, tiles - 1), 0)) for i in range(count)],
                pl.BlockSpec(w.shape, lambda r, tab: (0, 0), pipeline_mode=pl.Buffered(1)),
                table,
                table,
                *[anywhere] * len(bufs),
            ],
            out_specs=[tokens, tokens, pl.BlockSpec((heads, HEAD, ROWS), lambda r, tab: (0, 0, tab[r]))],
        ),
        out_shape=[jax.ShapeDtypeStruct(s, w.dtype) for s in shapes],
        input_output_aliases={count + 4 + i: i for i in range(len(bufs))},
        compiler_params=pltpu.CompilerParams(dimension_semantics=("arbitrary",), vmem_limit_bytes=VMEM),
        cost_estimate=pl.CostEstimate(
            flops=2 * count * rows * depth * w.shape[1], transcendentals=0, bytes_accessed=2 * (count * rows * (depth + w.shape[1]) + w.size)
        ),
        name="qkv",
    )(tab, *xs, w, cos, sin, *bufs)


def _attend_kernel(tab_ref, q_ref, k_ref, vt_ref, *rest, scale, carried, keep, modes):
    st_in = rest[0] if carried else None
    outs, (top_s, mix_s) = rest[carried:-2], rest[-2:]
    heads, rows = q_ref.shape[0], q_ref.shape[1]
    _, _, mode, start, end = (tab_ref[i, pl.program_id(0)] for i in range(5))
    e = scale * LOG2E
    low = jnp.bfloat16

    def fresh():
        for h in range(heads):
            top_s[h : h + 1, :] = jnp.full((1, rows), NEG, jnp.float32)
            mix_s[h] = jnp.zeros((HEAD + 8, rows), jnp.float32)

    def resume():
        for h in range(heads):
            mix_s[h] = st_in[0, h, : HEAD + 8, :]
            top_s[h : h + 1, :] = st_in[0, h, HEAD + 8 : HEAD + 9, :]

    pl.when(start == 1)(fresh)
    if carried:
        pl.when(start == 2)(resume)

    def block(pieces):
        scores = [_dot(k_ref[h, lo : lo + keys, :], q_ref[h, at : at + STRIP, :], 1, 1) for h, at, lo, keys, _ in pieces]
        weights, keeps = [], []
        for (h, at, lo, _, masked), s in zip(pieces, scores):
            if masked:
                seen = lax.broadcasted_iota(jnp.int32, s.shape, 1) + (at - lo) >= lax.broadcasted_iota(jnp.int32, s.shape, 0)
                s = jnp.where(seen, s, HIDDEN)
            old = top_s[h : h + 1, at : at + STRIP]
            top = jnp.maximum(old, s.max(axis=0, keepdims=True))
            top_s[h : h + 1, at : at + STRIP] = top
            weights.append(jnp.exp2((s - top) * e).astype(low))
            keeps.append(jnp.exp2((old - top) * e))
        for (h, at, lo, keys, _), p, keep in zip(pieces, weights, keeps):
            values = jnp.concatenate([vt_ref[h, :, lo : lo + keys], jnp.ones((8, keys), low)], axis=0)
            mix_s[h, :, at : at + STRIP] = mix_s[h, :, at : at + STRIP] * keep + _dot(values, p, 1, 0)

    def whole():
        for lo in range(0, rows, KEYS):
            block([(h, at, lo, KEYS, False) for h in range(heads) for at in range(0, rows, STRIP)])

    def cut():
        for lo in range(0, rows, CUT):
            block([(h, at, lo, CUT, at < lo + CUT) for h in range(heads) for at in range(0, rows, STRIP) if at + STRIP > lo])

    if 1 in modes:
        pl.when(mode == 1)(whole)
    if 2 in modes:
        pl.when(mode == 2)(cut)

    if keep:

        @pl.when(end == 1)
        def _():
            for h in range(heads):
                outs[0][0, h, : HEAD + 8, :] = mix_s[h]
                outs[0][0, h, HEAD + 8 :, :] = jnp.broadcast_to(top_s[h : h + 1, :], (8, rows))

    for i, o_ref in enumerate(outs[keep:]):

        @pl.when(end == 2 + i)
        def _():
            for h in range(heads):
                out = (mix_s[h, :HEAD, :] * (1 / mix_s[h, HEAD : HEAD + 1, :])).T
                o_ref[:, h * HEAD : (h + 1) * HEAD] = out.astype(low)


def _items(rows, finals):
    items = []
    for i, keys, fresh in rows:
        keys = [j for j in keys if j <= i]
        if not keys and i not in finals:
            continue
        mine = [[i, j, 2 if j == i else 1, 0, 0] for j in keys] or [[i, i, 0, 0, 0]]
        mine[0][3] = 1 if fresh else 2
        mine[-1][4] = 2 + finals.index(i) if i in finals else 1
        items += mine
    return items


def attend(me, plans, bufs, state=None, keep=True):
    q, k, vt = bufs
    heads, tokens = q.shape[0], q.shape[1]
    rows = BLOCK
    lists = [_items(*p) for p in plans]
    modes = {item[2] for items in lists for item in items}
    steps = max(len(items) for items in lists)
    lists = [items + [items[-1][:2] + [0, 0, 0]] * (steps - len(items)) for items in lists]
    tab = lax.dynamic_index_in_dim(jnp.asarray(lists, jnp.int32).transpose(0, 2, 1), me, 0, False)
    carried = state is not None
    st_spec = pl.BlockSpec((1, heads, HEAD + 16, rows), lambda s, tab: (tab[0, s], 0, 0, 0))
    in_specs = [
        pl.BlockSpec((heads, rows, HEAD), lambda s, tab: (0, tab[0, s], 0)),
        pl.BlockSpec((heads, rows, HEAD), lambda s, tab: (0, tab[1, s], 0)),
        pl.BlockSpec((heads, HEAD, rows), lambda s, tab: (0, 0, tab[1, s])),
    ]
    given = [q, k, vt]
    if carried:
        given.append(state)
        in_specs.append(st_spec)
    n = len(plans[0][1])
    out_specs = [st_spec] * keep + [pl.BlockSpec((rows, heads * HEAD), lambda s, tab: (0, 0))] * n
    out_shape = [jax.ShapeDtypeStruct((tokens // rows, heads, HEAD + 16, rows), jnp.float32)] * keep
    out_shape += [jax.ShapeDtypeStruct((rows, heads * HEAD), jnp.bfloat16)] * n
    work = steps * heads * rows * rows
    return pl.pallas_call(
        functools.partial(_attend_kernel, scale=HEAD**-0.5, carried=carried, keep=keep, modes=modes),
        grid_spec=pltpu.PrefetchScalarGridSpec(
            num_scalar_prefetch=1,
            grid=(steps,),
            in_specs=in_specs,
            out_specs=out_specs,
            scratch_shapes=[pltpu.VMEM((heads, rows), jnp.float32), pltpu.VMEM((heads, HEAD + 8, rows), jnp.float32)],
        ),
        out_shape=out_shape,
        input_output_aliases={4: 0} if carried and keep else {},
        compiler_params=pltpu.CompilerParams(dimension_semantics=("arbitrary",), vmem_limit_bytes=VMEM),
        cost_estimate=pl.CostEstimate(flops=4 * work * HEAD, transcendentals=work, bytes_accessed=2**24),
        name="attend",
    )(tab, *given)


def _out_kernel(ids_ref, *refs, count, first):
    base, o_refs, w_refs = refs[0], refs[first : first + count], refs[first + count : first + 2 * count]
    y_ref = refs[-1]
    acc = None
    for o_ref, w_ref in zip(o_refs, w_refs):
        part = _dot(o_ref[...], w_ref[...], 1, 0)
        acc = part if acc is None else acc + part
    if first == 2:
        acc = refs[1][...] + acc
    if first:
        acc = base[...].astype(jnp.float32) + acc
    y_ref[...] = acc.astype(y_ref.dtype)


def project(ids, parts, wo, rest=None):
    (rows, width), depth, count = parts[0].shape, wo.shape[1], len(parts)
    tiles = rows // ROWS
    given = [*parts, *[wo] * count]
    specs = [pl.BlockSpec((ROWS, width), lambda r, ids: (r, 0))] * count
    specs += [pl.BlockSpec((width, depth), lambda r, ids, n=n: (ids[n], 0), pipeline_mode=pl.Buffered(1)) for n in range(count)]
    out, at, alias, first = jax.ShapeDtypeStruct((rows, depth), jnp.float32), lambda r, ids: (r, 0), {}, 0
    if rest is not None:
        x, total, half, y = rest
        at, before = lambda r, ids: (half * tiles + r, 0), [x] if total is None else [x, total]
        first = len(before)
        given = [*before, *given]
        specs = [pl.BlockSpec((ROWS, depth), at), pl.BlockSpec((ROWS, depth), lambda r, ids: (r, 0))][:first] + specs
        out = jax.ShapeDtypeStruct(x.shape, x.dtype)
        if y is not None:
            alias = {1 + len(given): 0}
            given.append(y)
            specs.append(pl.BlockSpec(memory_space=pl.ANY))
    return pl.pallas_call(
        functools.partial(_out_kernel, count=count, first=first),
        grid_spec=pltpu.PrefetchScalarGridSpec(
            num_scalar_prefetch=1, grid=(tiles,), in_specs=specs, out_specs=pl.BlockSpec((ROWS, depth), at)
        ),
        out_shape=out,
        input_output_aliases=alias,
        compiler_params=pltpu.CompilerParams(dimension_semantics=("arbitrary",), vmem_limit_bytes=VMEM),
        cost_estimate=pl.CostEstimate(
            flops=2 * rows * count * width * depth, transcendentals=0, bytes_accessed=4 * rows * depth + 2 * count * width * depth
        ),
        name="project",
    )(ids, *given)


def _place_kernel(tab_ref, *refs, owned):
    out_ref, sems = refs[-2:]
    columns, copies = out_ref.shape[2] // owned[0], []

    def send(piece, there):
        copies.append(pltpu.make_async_copy(piece, there, sems.at[len(copies)]))
        copies[-1].start()

    for j, ref in enumerate(refs[: owned[0]]):
        rows = ref.shape[0] // owned[1]
        for i in range(owned[1]):
            send(ref.at[i * rows : (i + 1) * rows], out_ref.at[tab_ref[i], :, j * columns : (j + 1) * columns])
    at = owned[1]
    for ref in refs[owned[0] : -2]:
        for i in range(ref.shape[0]):
            send(ref.at[i], out_ref.at[tab_ref[at]])
            at += 1
    for copy in copies:
        copy.wait()


def place(slots, own, arrays):
    count, rows, columns = len(slots), *arrays[0].shape[1:]
    tab = jnp.stack([jnp.asarray(s, jnp.int32) for s in [*slots, own[0][1]]])
    owned = (len(own), count - sum(len(t) for t in arrays))
    whole = lambda t: pl.BlockSpec(t.shape, lambda i, tab: (0,) * t.ndim)
    out = jax.ShapeDtypeStruct((count, rows, columns), arrays[0].dtype)
    return pl.pallas_call(
        functools.partial(_place_kernel, owned=owned),
        grid_spec=pltpu.PrefetchScalarGridSpec(
            num_scalar_prefetch=1,
            grid=(1,),
            in_specs=[
                *[pl.BlockSpec((w.shape[0], columns // len(own)), lambda i, tab: (0, tab[count])) for w, _ in own],
                *[whole(t) for t in arrays],
            ],
            out_specs=pl.BlockSpec(memory_space=pl.ANY),
            scratch_shapes=[pltpu.SemaphoreType.DMA((count + len(own) * owned[1],))],
        ),
        out_shape=out,
        compiler_params=pltpu.CompilerParams(vmem_limit_bytes=VMEM),
        cost_estimate=pl.CostEstimate(flops=2**24, transcendentals=0, bytes_accessed=4 * count * rows * columns),
        name="place",
    )(tab, *[w for w, _ in own], *arrays).reshape(count * rows, columns)


def solution(mesh):
    n, groups = mesh.shape["sp"], mesh.shape["dp"]
    right = [(i, (i + 1) % n) for i in range(n)]
    left = [(i, (i - 1) % n) for i in range(n)]
    over = [(i, (i + 2) % n) for i in range(n)]
    pair = [(i, i ^ 1) for i in range(groups)]
    quad = [(i, i ^ 2) for i in range(groups)]

    def step(x, gain, wq, wk, wv, wo):
        own, _ = x.shape
        share = wq.shape[0]
        width = wq.shape[1] // n
        me, lot = lax.axis_index("sp"), lax.axis_index("dp") % 4
        lft, rgt, opp = (me + n - 1) % n, (me + 1) % n, (me + 2) % n
        bit = share // 4

        def gathered(t, cut):
            ways = ((rgt, right), (lft, left), (opp, over))
            a = jnp.stack([lax.ppermute(cut(t, d), "sp", p) for d, p in ways])
            b = lax.ppermute(a, "dp", quad)
            return [a, b, lax.ppermute(a, "dp", pair), lax.ppermute(b, "dp", pair)]

        slots = [me * 4 + i for i in range(4)]
        slots += [d * 4 + c for c in (lot, lot ^ 2, lot ^ 1, lot ^ 3) for d in (lft, rgt, opp)]

        def columns(ws, dev):
            cut = lax.dynamic_slice_in_dim(ws, dev * width, width, 2)
            return cut.transpose(1, 0, 2).reshape(ws.shape[1], 3 * width)

        mine = jnp.stack([lax.dynamic_slice_in_dim(w, lot * bit, bit, 0) for w in (wq, wk, wv)])
        parts = gathered(mine, columns)
        w = place(slots, [(wq, me), (wk, me), (wv, me)], parts)

        piece = own // 4
        a = [normed(x[i * piece : (i + 1) * piece], gain) for i in range(4)]
        l, r, o = [None] * 4, [None] * 4, [None] * 4
        for way in (0, 2):
            l[way], r[way + 1] = lax.ppermute(a[way], "sp", right), lax.ppermute(a[way + 1], "sp", left)
            l[way + 1], r[way] = lax.ppermute(a[way + 1], "sp", right), lax.ppermute(a[way], "sp", left)
            o[way], o[way + 1] = lax.ppermute(l[way], "sp", right), lax.ppermute(r[way + 1], "sp", left)

        tokens = n * own
        rate = THETA ** (-jnp.arange(HEAD // 2, dtype=jnp.float32) / (HEAD // 2))
        big = jnp.arange(0, tokens, 128, dtype=jnp.float32)[:, None, None] * rate
        small = jnp.arange(128, dtype=jnp.float32)[None, :, None] * rate
        cb, sb, cs, ss = lax.optimization_barrier((jnp.cos(big), jnp.sin(big), jnp.cos(small), jnp.sin(small)))
        cos, sin = (cb * cs - sb * ss).reshape(tokens, -1), (sb * cs + cb * ss).reshape(tokens, -1)

        def make(*pieces, bufs):
            return qkv([d * own + i * piece for d, _, i in pieces], [t[i] for _, t, i in pieces], w, cos, sin, bufs)

        ring = [[[2 * d, 2 * d + 1] for d in (m, (m - 1) % n, (m + 1) % n, (m + 2) % n)] for m in range(n)]
        old = lambda rows, keys: [(i, keys, False) for i in rows]
        new = lambda rows, keys: [(i, keys, True) for i in rows]
        plan = lambda f: [f(*blocks) for blocks in ring]
        bufs = make(*[(me, a, i) for i in range(4)], bufs=[])
        (state,) = attend(me, plan(lambda o, l, r, c: (new(o, o), [])), bufs)
        bufs = make((lft, l, 0), (lft, l, 1), (rgt, r, 0), (rgt, r, 1), bufs=bufs)
        (state,) = attend(me, plan(lambda o, l, r, c: (old(o, [l[0], r[0]]) + new([l[0], r[0]], [*o, l[0], r[0]]), [])), bufs, state)
        bufs = make((lft, l, 2), (rgt, r, 3), bufs=bufs)
        bufs = make((lft, l, 3), (rgt, r, 2), bufs=bufs)
        (state,) = attend(me, plan(lambda o, l, r, c: (old([*o, l[0], r[0]], [l[1], r[1]]) + new([l[1], r[1]], [*o, *l, *r]), [])), bufs, state)
        bufs = make((opp, o, 0), (opp, o, 1), bufs=bufs)
        last = plan(lambda o, l, r, c: (old([*o, *l, *r], [c[0]]) + new([c[0]], [*o, *l, *r, c[0]]), [c[0]]))
        state, first_opp = attend(me, last, bufs, state)
        bufs = make((opp, o, 2), (opp, o, 3), bufs=bufs)

        def spread(call, o, l, r, c):
            keys = [j for j in range(c[1] + 1)]
            cuts = {0: (0, 0), 1: (1, 2), 2: (1, 2), 3: (2, 4)}[c[0] // 2]
            if call == 2:
                rows = old(o, [c[1]]) + [(c[1], keys[cuts[1] :], cuts[1] == 0)]
                return rows, [*o, c[1]]
            rows = old([r[call], l[call]], [c[1]])
            now = keys[cuts[0] : cuts[1]] if call else keys[: cuts[0]]
            return rows + [(c[1], now, call == 0)], [r[call], l[call]]

        sides = []
        for h in range(2):
            state, *got = attend(me, plan(functools.partial(spread, h)), bufs, state)
            sides.append(got)
        rest = attend(me, plan(functools.partial(spread, 2)), bufs, state, False)
        to_opp, kept = [first_opp, rest[2]], rest[:2]

        parts = gathered(lax.dynamic_slice_in_dim(wo, lot * bit, bit, 0), lambda t, d: t)
        full = place(slots, [(wo, 0)], parts)

        ids, far = jnp.stack([me, lft, rgt]).astype(jnp.int32), opp.astype(jnp.int32).reshape(1)
        near, sent = [], []
        for h in range(2):
            near.append([kept[h], lax.ppermute(sides[h][0], "sp", right), lax.ppermute(sides[h][1], "sp", left)])
        for h in range(2):
            sent.append(lax.ppermute(to_opp[h], "sp", over))
        y = project(jnp.concatenate([ids, far]), [*near[0], sent[0]], full, (x, None, 0, None))
        y = project(jnp.concatenate([ids, far]), [*near[1], sent[1]], full, (x, None, 1, y))
        return y

    tokens, whole = P(("dp", "sp"), None), P("sp", None)
    return jax.shard_map(
        step,
        mesh=mesh,
        in_specs=(tokens, P(None), whole, whole, whole, whole),
        out_specs=tokens,
        check_vma=False,
    )
```

```python
import functools

import jax
import jax.numpy as jnp
from jax import lax
from jax.experimental import pallas as pl
from jax.experimental.pallas import tpu as pltpu
from jax.sharding import PartitionSpec as P


HEAD = 256
THETA = 10000
NEG = -1e30
HIDDEN = 2 * NEG
LOG2E = 1.4426950408889634
VMEM = 56 * 2**20
STRIP = 512
KEYS = 512
CUT = 512
BLOCK = 1024
ROWS = 256


def _dot(a, b, ca, cb):
    return lax.dot_general(a, b, (((ca,), (cb,)), ((), ())), preferred_element_type=jnp.float32)


def normed(x, gain):
    wide = x.astype(jnp.float32)
    scale = lax.rsqrt(jnp.mean(wide * wide, -1, keepdims=True) + 1e-6)
    return (wide * scale * gain.astype(jnp.float32)).astype(jnp.bfloat16)


def _qkv_kernel(tab_ref, *refs, count, tiles):
    a_refs, (w_ref, cos_ref, sin_ref), (q_ref, k_ref, vt_ref) = refs[:count], refs[count : count + 3], refs[-3:]
    heads = q_ref.shape[0]
    half, width = HEAD // 2, heads * HEAD
    a = a_refs[0][...]
    for i in range(1, count):
        a = jnp.where(pl.program_id(0) < i * tiles, a, a_refs[i][...])
    cos, sin = cos_ref[...], sin_ref[...]
    for n, ref in enumerate((q_ref, k_ref)):
        t = _dot(a, w_ref[:, n * width : (n + 1) * width], 1, 0).astype(jnp.bfloat16).astype(jnp.float32)
        for h in range(heads):
            lo, hi = t[:, h * HEAD : h * HEAD + half], t[:, h * HEAD + half : (h + 1) * HEAD]
            ref[h, :, :half] = (lo * cos - hi * sin).astype(jnp.bfloat16)
            ref[h, :, half:] = (hi * cos + lo * sin).astype(jnp.bfloat16)
    v = _dot(a, w_ref[:, 2 * width :], 1, 0).astype(jnp.bfloat16)
    for h in range(heads):
        vt_ref[h] = v[:, h * HEAD : (h + 1) * HEAD].T


def qkv(firsts, xs, w, cos, sin, bufs):
    rows, depth = xs[0].shape
    heads = w.shape[1] // (3 * HEAD)
    shapes = [(heads, len(cos), HEAD), (heads, len(cos), HEAD), (heads, HEAD, len(cos))]
    tiles, count = rows // ROWS, len(xs)
    tab = jnp.stack([f // ROWS + t for f in firsts for t in range(tiles)]).astype(jnp.int32)
    table = pl.BlockSpec((ROWS, HEAD // 2), lambda r, tab: (tab[r], 0))
    anywhere = pl.BlockSpec(memory_space=pl.ANY)
    tokens = pl.BlockSpec((heads, ROWS, HEAD), lambda r, tab: (0, tab[r], 0))
    return pl.pallas_call(
        functools.partial(_qkv_kernel, count=count, tiles=tiles),
        grid_spec=pltpu.PrefetchScalarGridSpec(
            num_scalar_prefetch=1,
            grid=(tiles * count,),
            in_specs=[
                *[pl.BlockSpec((ROWS, depth), lambda r, tab, i=i: (jnp.clip(r - i * tiles, 0, tiles - 1), 0)) for i in range(count)],
                pl.BlockSpec(w.shape, lambda r, tab: (0, 0), pipeline_mode=pl.Buffered(1)),
                table,
                table,
                *[anywhere] * len(bufs),
            ],
            out_specs=[tokens, tokens, pl.BlockSpec((heads, HEAD, ROWS), lambda r, tab: (0, 0, tab[r]))],
        ),
        out_shape=[jax.ShapeDtypeStruct(s, w.dtype) for s in shapes],
        input_output_aliases={count + 4 + i: i for i in range(len(bufs))},
        compiler_params=pltpu.CompilerParams(dimension_semantics=("arbitrary",), vmem_limit_bytes=VMEM),
        cost_estimate=pl.CostEstimate(
            flops=2 * count * rows * depth * w.shape[1], transcendentals=0, bytes_accessed=2 * (count * rows * (depth + w.shape[1]) + w.size)
        ),
        name="qkv",
    )(tab, *xs, w, cos, sin, *bufs)


def _attend_kernel(tab_ref, q_ref, k_ref, vt_ref, *rest, scale, carried, keep, modes):
    st_in = rest[0] if carried else None
    outs, (top_s, mix_s) = rest[carried:-2], rest[-2:]
    heads, rows = q_ref.shape[0], q_ref.shape[1]
    _, _, mode, start, end = (tab_ref[i, pl.program_id(0)] for i in range(5))
    e = scale * LOG2E
    low = jnp.bfloat16

    def fresh():
        for h in range(heads):
            top_s[h : h + 1, :] = jnp.full((1, rows), NEG, jnp.float32)
            mix_s[h] = jnp.zeros((HEAD + 8, rows), jnp.float32)

    def resume():
        for h in range(heads):
            mix_s[h] = st_in[0, h, : HEAD + 8, :]
            top_s[h : h + 1, :] = st_in[0, h, HEAD + 8 : HEAD + 9, :]

    pl.when(start == 1)(fresh)
    if carried:
        pl.when(start == 2)(resume)

    def block(pieces):
        scores = [_dot(k_ref[h, lo : lo + keys, :], q_ref[h, at : at + STRIP, :], 1, 1) for h, at, lo, keys, _ in pieces]
        weights, keeps = [], []
        for (h, at, lo, _, masked), s in zip(pieces, scores):
            if masked:
                seen = lax.broadcasted_iota(jnp.int32, s.shape, 1) + (at - lo) >= lax.broadcasted_iota(jnp.int32, s.shape, 0)
                s = jnp.where(seen, s, HIDDEN)
            old = top_s[h : h + 1, at : at + STRIP]
            top = jnp.maximum(old, s.max(axis=0, keepdims=True))
            top_s[h : h + 1, at : at + STRIP] = top
            weights.append(jnp.exp2((s - top) * e).astype(low))
            keeps.append(jnp.exp2((old - top) * e))
        for (h, at, lo, keys, _), p, keep in zip(pieces, weights, keeps):
            values = jnp.concatenate([vt_ref[h, :, lo : lo + keys], jnp.ones((8, keys), low)], axis=0)
            mix_s[h, :, at : at + STRIP] = mix_s[h, :, at : at + STRIP] * keep + _dot(values, p, 1, 0)

    def whole():
        for lo in range(0, rows, KEYS):
            block([(h, at, lo, KEYS, False) for h in range(heads) for at in range(0, rows, STRIP)])

    def cut():
        for lo in range(0, rows, CUT):
            block([(h, at, lo, CUT, at < lo + CUT) for h in range(heads) for at in range(0, rows, STRIP) if at + STRIP > lo])

    if 1 in modes:
        pl.when(mode == 1)(whole)
    if 2 in modes:
        pl.when(mode == 2)(cut)

    if keep:

        @pl.when(end == 1)
        def _():
            for h in range(heads):
                outs[0][0, h, : HEAD + 8, :] = mix_s[h]
                outs[0][0, h, HEAD + 8 :, :] = jnp.broadcast_to(top_s[h : h + 1, :], (8, rows))

    for i, o_ref in enumerate(outs[keep:]):

        @pl.when(end == 2 + i)
        def _():
            for h in range(heads):
                out = (mix_s[h, :HEAD, :] * (1 / mix_s[h, HEAD : HEAD + 1, :])).T
                o_ref[:, h * HEAD : (h + 1) * HEAD] = out.astype(low)


def _items(rows, finals):
    items = []
    for i, keys, fresh in rows:
        keys = [j for j in keys if j <= i]
        if not keys and i not in finals:
            continue
        mine = [[i, j, 2 if j == i else 1, 0, 0] for j in keys] or [[i, i, 0, 0, 0]]
        mine[0][3] = 1 if fresh else 2
        mine[-1][4] = 2 + finals.index(i) if i in finals else 1
        items += mine
    return items


def attend(me, plans, bufs, state=None, keep=True):
    q, k, vt = bufs
    heads, tokens = q.shape[0], q.shape[1]
    rows = BLOCK
    lists = [_items(*p) for p in plans]
    modes = {item[2] for items in lists for item in items}
    steps = max(len(items) for items in lists)
    lists = [items + [items[-1][:2] + [0, 0, 0]] * (steps - len(items)) for items in lists]
    tab = lax.dynamic_index_in_dim(jnp.asarray(lists, jnp.int32).transpose(0, 2, 1), me, 0, False)
    carried = state is not None
    st_spec = pl.BlockSpec((1, heads, HEAD + 16, rows), lambda s, tab: (tab[0, s], 0, 0, 0))
    in_specs = [
        pl.BlockSpec((heads, rows, HEAD), lambda s, tab: (0, tab[0, s], 0)),
        pl.BlockSpec((heads, rows, HEAD), lambda s, tab: (0, tab[1, s], 0)),
        pl.BlockSpec((heads, HEAD, rows), lambda s, tab: (0, 0, tab[1, s])),
    ]
    given = [q, k, vt]
    if carried:
        given.append(state)
        in_specs.append(st_spec)
    n = len(plans[0][1])
    out_specs = [st_spec] * keep + [pl.BlockSpec((rows, heads * HEAD), lambda s, tab: (0, 0))] * n
    out_shape = [jax.ShapeDtypeStruct((tokens // rows, heads, HEAD + 16, rows), jnp.float32)] * keep
    out_shape += [jax.ShapeDtypeStruct((rows, heads * HEAD), jnp.bfloat16)] * n
    work = steps * heads * rows * rows
    return pl.pallas_call(
        functools.partial(_attend_kernel, scale=HEAD**-0.5, carried=carried, keep=keep, modes=modes),
        grid_spec=pltpu.PrefetchScalarGridSpec(
            num_scalar_prefetch=1,
            grid=(steps,),
            in_specs=in_specs,
            out_specs=out_specs,
            scratch_shapes=[pltpu.VMEM((heads, rows), jnp.float32), pltpu.VMEM((heads, HEAD + 8, rows), jnp.float32)],
        ),
        out_shape=out_shape,
        input_output_aliases={4: 0} if carried and keep else {},
        compiler_params=pltpu.CompilerParams(dimension_semantics=("arbitrary",), vmem_limit_bytes=VMEM),
        cost_estimate=pl.CostEstimate(flops=4 * work * HEAD, transcendentals=work, bytes_accessed=2**24),
        name="attend",
    )(tab, *given)


def _out_kernel(tab_ref, x_ref, *refs, parts):
    o_refs, w_refs, (y_ref, w_s, sems) = refs[:4], refs[4 : 5 + parts], refs[-3:]
    bit = w_s.shape[1]

    @pl.when(pl.program_id(0) == 0)
    def _():
        copies = []
        for i in range(4):
            copies.append((w_refs[0].at[i * bit : (i + 1) * bit], i))
        for n, ref in enumerate(w_refs[1:]):
            copies += [(ref.at[i], 4 + n * 3 + i) for i in range(3)]
        copies = [pltpu.make_async_copy(piece, w_s.at[tab_ref[i]], sems.at[i]) for piece, i in copies]
        for copy in copies:
            copy.start()
        for copy in copies:
            copy.wait()

    acc = None
    for n, o_ref in enumerate(o_refs):
        part = _dot(o_ref[...], w_s[4 * n : 4 * n + 4].reshape(4 * bit, w_s.shape[2]), 1, 0)
        acc = part if acc is None else acc + part
    y_ref[...] = (x_ref[...].astype(jnp.float32) + acc).astype(y_ref.dtype)


def project(slots, x, sums, wo, parts, half, y):
    (rows, width), depth = sums[0].shape, wo.shape[1]
    tiles, bit = rows // ROWS, parts[0].shape[1]
    at = lambda r, tab: (half * tiles + r, 0)
    anywhere = pl.BlockSpec(memory_space=pl.ANY)
    given = [x, *sums, wo, *parts, *([] if y is None else [y])]
    return pl.pallas_call(
        functools.partial(_out_kernel, parts=len(parts)),
        grid_spec=pltpu.PrefetchScalarGridSpec(
            num_scalar_prefetch=1,
            grid=(tiles,),
            in_specs=[
                pl.BlockSpec((ROWS, depth), at),
                *[pl.BlockSpec((ROWS, width), lambda r, tab: (r, 0))] * 4,
                *[anywhere] * (len(given) - 5),
            ],
            out_specs=pl.BlockSpec((ROWS, depth), at),
            scratch_shapes=[pltpu.VMEM((len(slots), bit, depth), wo.dtype), pltpu.SemaphoreType.DMA((len(slots),))],
        ),
        out_shape=jax.ShapeDtypeStruct(x.shape, x.dtype),
        input_output_aliases={} if y is None else {len(given): 0},
        compiler_params=pltpu.CompilerParams(dimension_semantics=("arbitrary",), vmem_limit_bytes=VMEM),
        cost_estimate=pl.CostEstimate(flops=8 * rows * width * depth, transcendentals=0, bytes_accessed=4 * rows * depth + 8 * width * depth),
        name="project",
    )(jnp.stack(slots).astype(jnp.int32), *given)


def _place_kernel(tab_ref, *refs, owned):
    out_ref, sems = refs[-2:]
    columns, copies = out_ref.shape[2] // owned[0], []

    def send(piece, there):
        copies.append(pltpu.make_async_copy(piece, there, sems.at[len(copies)]))
        copies[-1].start()

    for j, ref in enumerate(refs[: owned[0]]):
        rows = ref.shape[0] // owned[1]
        for i in range(owned[1]):
            send(ref.at[i * rows : (i + 1) * rows], out_ref.at[tab_ref[i], :, j * columns : (j + 1) * columns])
    at = owned[1]
    for ref in refs[owned[0] : -2]:
        for i in range(ref.shape[0]):
            send(ref.at[i], out_ref.at[tab_ref[at]])
            at += 1
    for copy in copies:
        copy.wait()


def place(slots, own, arrays):
    count, rows, columns = len(slots), *arrays[0].shape[1:]
    tab = jnp.stack([jnp.asarray(s, jnp.int32) for s in [*slots, own[0][1]]])
    owned = (len(own), count - sum(len(t) for t in arrays))
    whole = lambda t: pl.BlockSpec(t.shape, lambda i, tab: (0,) * t.ndim)
    out = jax.ShapeDtypeStruct((count, rows, columns), arrays[0].dtype)
    return pl.pallas_call(
        functools.partial(_place_kernel, owned=owned),
        grid_spec=pltpu.PrefetchScalarGridSpec(
            num_scalar_prefetch=1,
            grid=(1,),
            in_specs=[
                *[pl.BlockSpec((w.shape[0], columns // len(own)), lambda i, tab: (0, tab[count])) for w, _ in own],
                *[whole(t) for t in arrays],
            ],
            out_specs=pl.BlockSpec(memory_space=pl.ANY),
            scratch_shapes=[pltpu.SemaphoreType.DMA((count + len(own) * owned[1],))],
        ),
        out_shape=out,
        compiler_params=pltpu.CompilerParams(vmem_limit_bytes=VMEM),
        cost_estimate=pl.CostEstimate(flops=2**24, transcendentals=0, bytes_accessed=4 * count * rows * columns),
        name="place",
    )(tab, *[w for w, _ in own], *arrays).reshape(count * rows, columns)


def solution(mesh):
    n, groups = mesh.shape["sp"], mesh.shape["dp"]
    right = [(i, (i + 1) % n) for i in range(n)]
    left = [(i, (i - 1) % n) for i in range(n)]
    over = [(i, (i + 2) % n) for i in range(n)]
    pair = [(i, i ^ 1) for i in range(groups)]
    quad = [(i, i ^ 2) for i in range(groups)]

    def step(x, gain, wq, wk, wv, wo):
        own, _ = x.shape
        share = wq.shape[0]
        width = wq.shape[1] // n
        me, lot = lax.axis_index("sp"), lax.axis_index("dp") % 4
        lft, rgt, opp = (me + n - 1) % n, (me + 1) % n, (me + 2) % n
        bit = share // 4

        def gathered(t, cut):
            ways = ((rgt, right), (lft, left), (opp, over))
            a = jnp.stack([lax.ppermute(cut(t, d), "sp", p) for d, p in ways])
            b = lax.ppermute(a, "dp", quad)
            return [a, b, lax.ppermute(a, "dp", pair), lax.ppermute(b, "dp", pair)]

        slots = [me * 4 + i for i in range(4)]
        slots += [d * 4 + c for c in (lot, lot ^ 2, lot ^ 1, lot ^ 3) for d in (lft, rgt, opp)]

        def columns(ws, dev):
            cut = lax.dynamic_slice_in_dim(ws, dev * width, width, 2)
            return cut.transpose(1, 0, 2).reshape(ws.shape[1], 3 * width)

        mine = jnp.stack([lax.dynamic_slice_in_dim(w, lot * bit, bit, 0) for w in (wq, wk, wv)])
        parts = gathered(mine, columns)
        w = place(slots, [(wq, me), (wk, me), (wv, me)], parts)

        piece = own // 4
        a = [normed(x[i * piece : (i + 1) * piece], gain) for i in range(4)]
        l, r, o = [None] * 4, [None] * 4, [None] * 4
        for way in (0, 2):
            l[way], r[way + 1] = lax.ppermute(a[way], "sp", right), lax.ppermute(a[way + 1], "sp", left)
            l[way + 1], r[way] = lax.ppermute(a[way + 1], "sp", right), lax.ppermute(a[way], "sp", left)
            o[way], o[way + 1] = lax.ppermute(l[way], "sp", right), lax.ppermute(r[way + 1], "sp", left)

        tokens = n * own
        rate = THETA ** (-jnp.arange(HEAD // 2, dtype=jnp.float32) / (HEAD // 2))
        big = jnp.arange(0, tokens, 128, dtype=jnp.float32)[:, None, None] * rate
        small = jnp.arange(128, dtype=jnp.float32)[None, :, None] * rate
        cb, sb, cs, ss = lax.optimization_barrier((jnp.cos(big), jnp.sin(big), jnp.cos(small), jnp.sin(small)))
        cos, sin = (cb * cs - sb * ss).reshape(tokens, -1), (sb * cs + cb * ss).reshape(tokens, -1)

        def make(*pieces, bufs):
            return qkv([d * own + i * piece for d, _, i in pieces], [t[i] for _, t, i in pieces], w, cos, sin, bufs)

        ring = [[[2 * d, 2 * d + 1] for d in (m, (m - 1) % n, (m + 1) % n, (m + 2) % n)] for m in range(n)]
        old = lambda rows, keys: [(i, keys, False) for i in rows]
        new = lambda rows, keys: [(i, keys, True) for i in rows]
        plan = lambda f: [f(*blocks) for blocks in ring]
        bufs = make(*[(me, a, i) for i in range(4)], bufs=[])
        (state,) = attend(me, plan(lambda o, l, r, c: (new(o, o), [])), bufs)
        bufs = make((lft, l, 0), (lft, l, 1), (rgt, r, 0), (rgt, r, 1), bufs=bufs)
        (state,) = attend(me, plan(lambda o, l, r, c: (old(o, [l[0], r[0]]) + new([l[0], r[0]], [*o, l[0], r[0]]), [])), bufs, state)
        bufs = make((lft, l, 2), (rgt, r, 3), bufs=bufs)
        bufs = make((lft, l, 3), (rgt, r, 2), bufs=bufs)
        (state,) = attend(me, plan(lambda o, l, r, c: (old([*o, l[0], r[0]], [l[1], r[1]]) + new([l[1], r[1]], [*o, *l, *r]), [])), bufs, state)
        bufs = make((opp, o, 0), (opp, o, 1), bufs=bufs)
        last = plan(lambda o, l, r, c: (old([*o, *l, *r], [c[0]]) + new([c[0]], [*o, *l, *r, c[0]]), [c[0]]))
        state, first_opp = attend(me, last, bufs, state)
        bufs = make((opp, o, 2), (opp, o, 3), bufs=bufs)

        def spread(call, o, l, r, c):
            keys = [j for j in range(c[1] + 1)]
            cuts = {0: (0, 0), 1: (1, 2), 2: (1, 2), 3: (2, 4)}[c[0] // 2]
            if call == 2:
                rows = old(o, [c[1]]) + [(c[1], keys[cuts[1] :], cuts[1] == 0)]
                return rows, [*o, c[1]]
            rows = old([r[call], l[call]], [c[1]])
            now = keys[cuts[0] : cuts[1]] if call else keys[: cuts[0]]
            return rows + [(c[1], now, call == 0)], [r[call], l[call]]

        sides = []
        for h in range(2):
            state, *got = attend(me, plan(functools.partial(spread, h)), bufs, state)
            sides.append(got)
        rest = attend(me, plan(functools.partial(spread, 2)), bufs, state, False)
        to_opp, kept = [first_opp, rest[2]], rest[:2]

        parts = gathered(lax.dynamic_slice_in_dim(wo, lot * bit, bit, 0), lambda t, d: t)
        fills = [jnp.int32(i) for i in range(4)]
        fills += [jnp.int32(4 * d) + c for c in (lot, lot ^ 2, lot ^ 1, lot ^ 3) for d in (1, 2, 3)]

        near, sent = [], []
        for h in range(2):
            near.append([kept[h], lax.ppermute(sides[h][0], "sp", right), lax.ppermute(sides[h][1], "sp", left)])
        for h in range(2):
            sent.append(lax.ppermute(to_opp[h], "sp", over))
        y = None
        for h in range(2):
            y = project(fills, x, [*near[h], sent[h]], wo, parts, h, y)
        return y

    tokens, whole = P(("dp", "sp"), None), P("sp", None)
    return jax.shard_map(
        step,
        mesh=mesh,
        in_specs=(tokens, P(None), whole, whole, whole, whole),
        out_specs=tokens,
        check_vma=False,
    )
```
